32 devices in a mesh: dp: 16 (over z, y, core), tp: 2 (over x).
Axes of the slice: x: 2, y: 2, z: 4, core: 2. Of those that a mesh axis runs over, the one named last changes fastest.
Arguments:
- decoder_rows: bfloat16 [16, 1024, 768], P('dp', 'tp'), may hold values from -16 to 16
- memory_rows: bfloat16 [16, 2048, 768], P('dp', 'tp'), may hold values from -6 to 6
- output_grad: bfloat16 [16, 1024, 768], P('dp', 'tp'), may hold values from -6 to 6
- token_segments: int32 [16, 1024], P('dp'), may hold values from 0 to 7, never falling along the last dimension, each value on 1 to 256 neighbouring positions
- memory_segments: int32 [16, 2048], P('dp'), may hold values from 0 to 7, never falling along the last dimension, each value on 1 to 512 neighbouring positions
- valid_mask: int32 [16, 1024], P('dp', 'tp'), may hold values from 0 to 1, as said below
- norm_gains: float32 [3, 768], replicated, may hold values from 0.5 to 1.5
- self_project: bfloat16 [3, 768, 768], P(None, None, 'tp'), may hold values from -0.21875 to 0.21875
- self_output: bfloat16 [768, 768], P('tp'), may hold values from -1.25 to 1.25
- cross_query: bfloat16 [768, 768], P(None, 'tp'), may hold values from -0.21875 to 0.21875
- cross_memory: bfloat16 [2, 768, 768], P(None, None, 'tp'), may hold values from -0.21875 to 0.21875
- cross_output: bfloat16 [768, 768], P('tp'), may hold values from -1.75 to 1.75
- gate_up: bfloat16 [2, 768, 2048], P(None, None, 'tp'), may hold values from -0.21875 to 0.21875
- down_weight: bfloat16 [2048, 768], P('tp'), may hold values from -0.125 to 0.125
Outputs:
- decoded: bfloat16 [16, 1024, 768], P('dp', 'tp')
- decoder_grad: float32 [16, 1024, 768], P('dp', 'tp')
- memory_grad: float32 [16, 2048, 768], P('dp', 'tp')
- root_squares: float32 [4], replicated
- gains_grad: float32 [3, 768], replicated
- self_project_grad: float32 [3, 768, 768], P(None, None, 'tp')
- self_output_grad: float32 [768, 768], P('tp')
- cross_query_grad: float32 [768, 768], P(None, 'tp')
- cross_memory_grad: float32 [2, 768, 768], P(None, None, 'tp')
- cross_output_grad: float32 [768, 768], P('tp')
- gate_up_grad: float32 [2, 768, 2048], P(None, None, 'tp')
- down_weight_grad: float32 [2048, 768], P('tp')
The draws below stay inside these ranges and needn't reach their ends.
Inputs may be any that keep to these rules, and one draw needn't show every extreme that they name: `token_segments`: segment ids never fall along a row, and every id of 0 to 7 occurs in every row. `memory_segments`: segment ids never fall along a row, and every id of 0 to 7 occurs in every row. `valid_mask`: in each row the valid tokens form a prefix of one token or more.
All inputs are finite; a program needn't handle non-finite values.
Results may differ from the reference program's by a relative error of at most 0.019.
The reference program's roundings to bfloat16 on the way count: a program that leaves them out, or rounds other values in their place, can miss the bound.
Values may be sent and summed in bfloat16 or wider, within the bound.
No kernel may reach another device: no remote copies, remote signals or barrier semaphores. Data moves between devices by JAX's collectives and lax.ppermute only.
A program may use at most 320 MiB of HBM per device.

```python
import math
import jax
import jax.numpy as jnp
import numpy as np
from jax import lax

D = 768
HEADS = 12
HD = 64
FF = 2048
INNER = 768
SEQ = 1024
MEM = 2048
SEGS = 8
ROWS = 16


def draw_decoder_rows(key, part):
    first = jax.random.fold_in(key, 0)
    rising = 1.0 + 2.0 * jnp.arange(ROWS, dtype=jnp.float32) / max(ROWS - 1, 1)
    values = 0.6 * jnp.clip(jax.random.normal(first, (ROWS, SEQ, D), jnp.float32), -6.0, 6.0) * rising[:, None, None]
    return values.astype(jnp.bfloat16)


def draw_valid_mask(key, part):
    row_index = jnp.arange(ROWS, dtype=jnp.int32)
    base_length = SEQ // 3 + (SEQ - SEQ // 3) * row_index // max(ROWS - 1, 1)
    jitter = jax.random.randint(key, (ROWS,), 0, SEQ // 8 + 1, dtype=jnp.int32)
    lengths = jnp.maximum(base_length - jitter, 1)
    positions = jnp.arange(SEQ, dtype=jnp.int32)
    return (positions[None, :] < lengths[:, None]).astype(jnp.int32)


def levels(key, shape, cuts, smallest, largest):
    loudness, own = 1.0, jax.random.fold_in(key, 6)
    for position, shards_of in cuts:
        steps = jnp.exp(jax.random.uniform(jax.random.fold_in(own, position), (shards_of,), jnp.float32, smallest / len(cuts), largest / len(cuts)))
        loudness = loudness * jnp.repeat(steps, shape[position] // shards_of).reshape([-1 if axis == position else 1 for axis in range(len(shape))])
    return loudness


def split_up(amount, total, bound, skew):
    weights = [(1 << 20) // math.isqrt(standing ** skew) + 1 for standing in range(2, amount + 1)]
    spare, holding = total - bound - (amount - 1), [1] * (amount - 1)
    while spare > 0:
        movable = [i for i in range(amount - 1) if holding[i] < bound]
        pool, left = sum([weights[i] for i in movable]), spare
        for i in movable:
            addition = min(bound - holding[i], max(1, left * weights[i] // pool), spare)
            holding[i] = holding[i] + addition
            spare = spare - addition
    return np.array([bound] + holding)


def ragged_sizes(key, amount, total, limit, lean):
    if amount == 2:
        one = jax.random.randint(key, (), max(1, total - limit), min(limit, total - 1) + 1)
        return jnp.stack([one, total - one])
    sizes = jnp.asarray(split_up(amount, total, limit, lean), jnp.int32)
    pairs = (amount - 1) // 2
    donor, taker = sizes[1:1 + 2 * pairs:2], sizes[2:2 + 2 * pairs:2]
    room = jnp.minimum(donor - 1, limit - taker)
    shifted = jax.random.randint(jax.random.fold_in(key, 1), (pairs,), 0, 1 << 20) % (room + 1)
    sizes = sizes.at[1:1 + 2 * pairs:2].set(donor - shifted).at[2:2 + 2 * pairs:2].set(taker + shifted)
    return sizes[jax.random.permutation(jax.random.fold_in(key, 2), amount)]


def centred(rng, dims, deviation, limit, cuts=(), kind=jnp.bfloat16):
    drawn = deviation * jax.random.normal(rng, dims, jnp.float32)
    if cuts:
        drawn = drawn * levels(rng, dims, cuts, -0.22, 0.18)
    return jnp.clip(drawn, -limit, limit).astype(kind)


def setup_inputs(seed: int = 0) -> dict:
    arg_keys = jax.random.split(jax.random.key(seed), 15)
    return {
        "decoder_rows": draw_decoder_rows(jax.random.fold_in(arg_keys[14], 71), 0),
        "memory_rows": centred(arg_keys[1], (ROWS, MEM, D), 1.0, 6.0, ((0, 16), (1, 2))),
        "output_grad": centred(arg_keys[2], (ROWS, SEQ, D), 1.0, 6.0, ((0, 16), (1, 2))),
        "token_segments": jax.vmap(lambda own: jnp.searchsorted(jnp.cumsum(ragged_sizes(own, SEGS, SEQ, SEQ // 4, 2)), jnp.arange(SEQ), side="right"))(jax.random.split(arg_keys[3], ROWS)).reshape((ROWS, SEQ)).astype(jnp.int32),
        "memory_segments": jax.vmap(lambda own: jnp.searchsorted(jnp.cumsum(ragged_sizes(own, SEGS, MEM, MEM // 4, 2)), jnp.arange(MEM), side="right"))(jax.random.split(arg_keys[4], ROWS)).reshape((ROWS, MEM)).astype(jnp.int32),
        "valid_mask": draw_valid_mask(jax.random.fold_in(arg_keys[14], 71), 0),
        "norm_gains": jnp.clip(1.0 + 0.1 * jax.random.normal(arg_keys[6], (3, D), jnp.float32), 0.5, 1.5),
        "self_project": centred(arg_keys[7], (3, D, INNER), D ** -0.5, 0.21875, ((2, 2),)),
        "self_output": centred(arg_keys[8], (INNER, D), (max(INNER * SEGS // (SEQ // 4), 1)) ** -0.5, 1.25, ((0, 2),)),
        "cross_query": centred(arg_keys[9], (D, INNER), D ** -0.5, 0.21875, ((1, 2),)),
        "cross_memory": centred(arg_keys[10], (2, D, INNER), D ** -0.5, 0.21875, ((2, 2),)),
        "cross_output": centred(arg_keys[11], (INNER, D), (max(INNER * SEGS // (MEM // 4), 1)) ** -0.5, 1.75, ((0, 2),)),
        "gate_up": centred(arg_keys[12], (2, D, FF), D ** -0.5, 0.21875, ((2, 2),)),
        "down_weight": centred(arg_keys[13], (FF, D), FF ** -0.5, 0.125, ((0, 2),)),
    }


@jax.custom_vjp
def low(v):
    return lax.optimization_barrier(v.astype(jnp.bfloat16)).astype(jnp.float32)

@jax.custom_vjp
def low_back(v):
    return v

def low_keep(v):
    return (low(v), None)

def low_pass(kept, grad):
    return (grad,)

def back_keep(v):
    return (v, None)

def back_low(kept, grad):
    return (low(grad),)
low.defvjp(low_keep, low_pass)
low_back.defvjp(back_keep, back_low)
HIGHEST = lax.Precision.HIGHEST

def rounded_both(value):
    return low(low_back(value))

def normalize(vector, factor):
    return vector * lax.rsqrt(lax.optimization_barrier(jnp.mean(vector * vector, axis=-1, keepdims=True)) + 1e-06) * factor

def split_heads(matrix):
    return matrix.reshape(matrix.shape[0], matrix.shape[1], HEADS, HD)

def join_heads(tensor):
    return tensor.reshape(tensor.shape[0], tensor.shape[1], HEADS * HD)

def attend(queries, key_rows, values, mask_table):
    score_scale = HD ** (-0.5)
    scores = jnp.einsum('gshe,gthe->ghst', queries, key_rows, precision=HIGHEST) * score_scale
    scores = low_back(scores)
    scores = jnp.where(mask_table[:, None], scores, -1e+30)
    attn_probs = low(jax.nn.softmax(scores, axis=-1))
    return jnp.einsum('ghst,gthe->gshe', attn_probs, values, precision=HIGHEST)

def decoder_layer(resid_in, memory, gains, self_project, self_output, cross_query, cross_memory, cross_output, gate_up, down_weight, self_mask, cross_mask):
    normed_a = low(normalize(resid_in, gains[0]))
    proj_a = rounded_both(jnp.einsum('gsd,cdi->cgsi', normed_a, self_project, precision=HIGHEST))
    att_a = rounded_both(join_heads(attend(split_heads(proj_a[0]), split_heads(proj_a[1]), split_heads(proj_a[2]), self_mask)))
    branch_a = low_back(jnp.einsum('gsi,id->gsd', att_a, self_output, precision=HIGHEST))
    resid1 = resid_in + branch_a
    normed_c = low(normalize(resid1, gains[1]))
    query_c = rounded_both(jnp.einsum('gsd,di->gsi', normed_c, cross_query, precision=HIGHEST))
    kv_c = rounded_both(jnp.einsum('gtd,cdi->cgti', memory, cross_memory, precision=HIGHEST))
    att_c = rounded_both(join_heads(attend(split_heads(query_c), split_heads(kv_c[0]), split_heads(kv_c[1]), cross_mask)))
    branch_c = low_back(jnp.einsum('gsi,id->gsd', att_c, cross_output, precision=HIGHEST))
    resid2 = resid1 + branch_c
    normed_m = low(normalize(resid2, gains[2]))
    gate_values = low_back(jnp.einsum('gsd,cdf->cgsf', normed_m, gate_up, precision=HIGHEST))
    hidden = low(jax.nn.gelu(gate_values[0], approximate=True) * gate_values[1])
    branch_m = low_back(jnp.einsum('gsf,fd->gsd', hidden, down_weight, precision=HIGHEST))
    return (resid2 + branch_m, (branch_a, branch_c, branch_m))

def reference(decoder_rows, memory_rows, output_grad, token_segments, memory_segments, valid_mask, norm_gains, self_project, self_output, cross_query, cross_memory, cross_output, gate_up, down_weight):
    group_rows = math.gcd(ROWS, max(1, 2048 // SEQ))
    group_count = ROWS // group_rows
    weights = tuple((matrix.astype(jnp.float32) for matrix in (norm_gains, self_project, self_output, cross_query, cross_memory, cross_output, gate_up, down_weight)))
    positions = jnp.arange(SEQ, dtype=jnp.int32)
    causal = positions[:, None] >= positions[None, :]

    def group_step(carried, inputs):
        group_input, group_memory, group_grad, group_tokens, group_patches, group_valid = inputs
        self_mask = (group_tokens[:, :, None] == group_tokens[:, None, :]) & causal[None]
        cross_mask = group_tokens[:, :, None] == group_patches[:, None, :]

        def forward(*primals):
            return decoder_layer(*primals, self_mask, cross_mask)
        output, pull_back, branches = jax.vjp(forward, group_input.astype(jnp.float32), group_memory.astype(jnp.float32), *weights, has_aux=True)
        valid_rows = group_valid.astype(jnp.float32)[..., None]
        gradients = pull_back(group_grad.astype(jnp.float32) * valid_rows)
        squares = jnp.stack([jnp.sum(output * output * valid_rows), jnp.sum(branches[0] * branches[0] * valid_rows), jnp.sum(branches[1] * branches[1] * valid_rows), jnp.sum(branches[2] * branches[2] * valid_rows), jnp.sum(valid_rows)])
        stat_sums, weight_sums = carried
        weight_sums = tuple((running + gradient for running, gradient in zip(weight_sums, gradients[2:])))
        return ((stat_sums + squares, weight_sums), (output.astype(jnp.bfloat16), gradients[0], gradients[1]))
    initial = (jnp.zeros((5,), jnp.float32), tuple((jnp.zeros(matrix.shape, jnp.float32) for matrix in weights)))
    inputs = (decoder_rows.reshape(group_count, group_rows, SEQ, D), memory_rows.reshape(group_count, group_rows, MEM, D), output_grad.reshape(group_count, group_rows, SEQ, D), token_segments.reshape(group_count, group_rows, SEQ), memory_segments.reshape(group_count, group_rows, MEM), valid_mask.reshape(group_count, group_rows, SEQ))
    (stat_sums, weight_sums), (decoded, decoder_grad, memory_grad) = lax.scan(group_step, initial, inputs)
    root_squares = jnp.sqrt(stat_sums[:4] / (stat_sums[4] * D))
    return (decoded.reshape(ROWS, SEQ, D), decoder_grad.reshape(ROWS, SEQ, D), memory_grad.reshape(ROWS, MEM, D), root_squares, weight_sums[0], weight_sums[1], weight_sums[2], weight_sums[3], weight_sums[4], weight_sums[5], weight_sums[6], weight_sums[7])
```

```python
import functools

import jax
import jax.numpy as jnp
from jax import lax
from jax.experimental import pallas as pl
from jax.experimental.pallas import tpu as pltpu
from jax.sharding import PartitionSpec as P

HD = 64
EPSILON = 1e-06
NEGATIVE = -1e30
BQ = 128
BK = 256
F32 = jnp.float32
BF16 = jnp.bfloat16


def rows_of_two_heads(block):
    lane = lax.broadcasted_iota(jnp.int32, block.shape, 1)
    zero = jnp.zeros_like(block)
    return jnp.concatenate([jnp.where(lane < HD, block, zero), jnp.where(lane >= HD, block, zero)], axis=0)


def heads_side_by_side(wide):
    return jnp.concatenate([wide[:HD, :BQ], wide[HD:, BQ:]], axis=0).T


def twice(row):
    return jnp.concatenate([row, row], axis=1)


def block_rows(ref, start):
    return ref[0, pl.ds(pl.multiple_of(start, BQ), BQ), :]


def forward_kernel(bounds, interval_ref, q_ref, *refs, n_parts, n_blocks, q_offset):
    key_refs, (out_ref, total_ref) = refs[: 2 * n_parts], refs[2 * n_parts :]
    key_iota = lax.broadcasted_iota(jnp.int32, (BK, 2 * BQ), 0)

    def one_block(b, _):
        queries = block_rows(q_ref, q_offset + b * BQ).astype(F32) * (HD**-0.5)
        q_wide = rows_of_two_heads(queries).T.astype(BF16)
        carry = (
            jnp.full((1, 2 * BQ), NEGATIVE, F32),
            jnp.zeros((1, 2 * BQ), F32),
            jnp.zeros((2 * HD, 2 * BQ), F32),
        )
        for part in range(n_parts):
            k_ref, v_ref = key_refs[2 * part], key_refs[2 * part + 1]
            first = twice(interval_ref[2 * part, pl.ds(b, 1), :])
            last = twice(interval_ref[2 * part + 1, pl.ds(b, 1), :])
            place = (part * n_blocks + b) * 2

            def step(j, carry, k_ref=k_ref, v_ref=v_ref, first=first, last=last):
                peak, total, acc = carry
                rows = pl.ds(pl.multiple_of(j * BK, BK), BK)
                scores = jnp.dot(k_ref[0, rows, :], q_wide, preferred_element_type=F32)
                seen = (key_iota >= first - j * BK) & (key_iota < last - j * BK)
                scores = jnp.where(seen, scores, NEGATIVE)
                new_peak = jnp.maximum(peak, jnp.max(scores, axis=0, keepdims=True))
                shrink = jnp.exp(peak - new_peak)
                probs = jnp.exp(scores - new_peak)
                total = total * shrink + jnp.sum(probs, axis=0, keepdims=True)
                acc = acc * shrink + lax.dot_general(
                    v_ref[0, rows, :], probs.astype(BF16), (((0,), (0,)), ((), ())), preferred_element_type=F32
                )
                return new_peak, total, acc

            carry = lax.fori_loop(bounds[place], bounds[place + 1], step, carry)
        peak, total, acc = carry
        out = heads_side_by_side(acc / total)
        out_ref[pl.ds(pl.multiple_of(b * BQ, BQ), BQ), :] = out.astype(BF16)
        total_ref[0, pl.ds(b, 1), :] = peak + jnp.log(total)
        return 0

    lax.fori_loop(0, n_blocks, one_block, 0)


def backward_kernel(bounds, interval_ref, total_ref, q_ref, out_ref, grad_ref, *refs, n_parts, n_blocks, q_offset, fused):
    key_refs, refs = refs[: 2 * n_parts], refs[2 * n_parts :]
    if fused:
        (dall_ref, dk_acc, dv_acc) = refs
    else:
        (dq_ref, dkv_ref, dk_acc, dv_acc) = refs
    key_iota = lax.broadcasted_iota(jnp.int32, (BK, 2 * BQ), 0)
    dk_acc[...] = jnp.zeros_like(dk_acc)
    dv_acc[...] = jnp.zeros_like(dv_acc)

    def one_block(b, _):
        queries = block_rows(q_ref, q_offset + b * BQ).astype(F32) * (HD**-0.5)
        q_rows = rows_of_two_heads(queries)
        q_wide = q_rows.T.astype(BF16)
        q_rows = q_rows.astype(BF16)
        here = pl.ds(pl.multiple_of(b * BQ, BQ), BQ)
        grad = grad_ref[here, :].astype(F32)
        g_rows = rows_of_two_heads(grad)
        g_wide = g_rows.T.astype(BF16)
        g_rows = g_rows.astype(BF16)
        product = (grad * out_ref[here, :].astype(F32)).T
        inner = jnp.concatenate(
            [jnp.sum(product[:HD], axis=0, keepdims=True), jnp.sum(product[HD:], axis=0, keepdims=True)], axis=1
        )
        log_total = total_ref[0, pl.ds(b, 1), :]
        dq = jnp.zeros((2 * HD, 2 * BQ), F32)
        base = 0
        for part in range(n_parts):
            k_ref, v_ref = key_refs[2 * part], key_refs[2 * part + 1]
            first = twice(interval_ref[2 * part, pl.ds(b, 1), :])
            last = twice(interval_ref[2 * part + 1, pl.ds(b, 1), :])
            place = (part * n_blocks + b) * 2

            def step(j, dq, k_ref=k_ref, v_ref=v_ref, first=first, last=last, base=base):
                rows = pl.ds(pl.multiple_of(j * BK, BK), BK)
                sums = pl.ds(pl.multiple_of(base + j * BK, BK), BK)
                keys = k_ref[0, rows, :]
                scores = jnp.dot(keys, q_wide, preferred_element_type=F32)
                prob_grad = jnp.dot(v_ref[0, rows, :], g_wide, preferred_element_type=F32)
                seen = (key_iota >= first - j * BK) & (key_iota < last - j * BK)
                probs = jnp.exp(jnp.where(seen, scores, NEGATIVE) - log_total)
                score_grad = (probs * (prob_grad - inner)).astype(BF16)
                dv_acc[sums, :] += jnp.dot(probs.astype(BF16), g_rows, preferred_element_type=F32)
                dk_acc[sums, :] += jnp.dot(score_grad, q_rows, preferred_element_type=F32)
                return dq + lax.dot_general(keys, score_grad, (((0,), (0,)), ((), ())), preferred_element_type=F32)

            dq = lax.fori_loop(bounds[place], bounds[place + 1], step, dq)
            base += k_ref.shape[1]
        dq = (heads_side_by_side(dq) * (HD**-0.5)).astype(BF16)
        if fused:
            dall_ref[0, pl.ds(pl.multiple_of(q_offset + b * BQ, BQ), BQ), :] = dq
        else:
            dq_ref[here, :] = dq
        return 0

    lax.fori_loop(0, n_blocks, one_block, 0)
    if fused:
        if q_offset:
            dall_ref[0, :q_offset, :] = jnp.zeros((q_offset, 2 * HD), BF16)
        dall_ref[1, :, :] = dk_acc[...].astype(BF16)
        dall_ref[2, :, :] = dv_acc[...].astype(BF16)
    else:
        dkv_ref[0, :, :] = dk_acc[...].astype(BF16)
        dkv_ref[1, :, :] = dv_acc[...].astype(BF16)


def column_block(array, index=None):
    if index is None:
        return pl.BlockSpec((array.shape[0], 2 * HD), lambda g, *_: (0, g))
    return pl.BlockSpec((1, array.shape[1], 2 * HD), lambda g, *_: (index, 0, g))


def whole(array):
    return pl.BlockSpec(array.shape, lambda g, *_: (0,) * array.ndim)


PARAMS = pltpu.CompilerParams(dimension_semantics=("arbitrary",), vmem_limit_bytes=48 << 20)


def attend_forward(plan, q, parts, q_offset):
    bounds, interval = plan
    q_array, q_index = q
    n_blocks, columns = interval.shape[1], q_array.shape[2]
    length, groups = n_blocks * BQ, columns // (2 * HD)
    operands, specs = [interval, q_array], [whole(interval), column_block(q_array, q_index)]
    for array, k_index, v_index in parts:
        operands += [array, array]
        specs += [column_block(array, k_index), column_block(array, v_index)]
    n_keys = sum(array.shape[1] for array, *_ in parts)
    return pl.pallas_call(
        functools.partial(forward_kernel, n_parts=len(parts), n_blocks=n_blocks, q_offset=q_offset),
        grid_spec=pltpu.PrefetchScalarGridSpec(
            num_scalar_prefetch=1,
            grid=(groups,),
            in_specs=specs,
            out_specs=[
                pl.BlockSpec((length, 2 * HD), lambda g, *_: (0, g)),
                pl.BlockSpec((1, n_blocks, 2 * BQ), lambda g, *_: (g, 0, 0)),
            ],
        ),
        out_shape=[
            jax.ShapeDtypeStruct((length, columns), BF16),
            jax.ShapeDtypeStruct((groups, n_blocks, 2 * BQ), F32),
        ],
        compiler_params=PARAMS,
        cost_estimate=pl.CostEstimate(
            flops=2 * length * n_keys * columns, bytes_accessed=4 * n_keys * columns, transcendentals=length * n_keys
        ),
        name="attend_forward",
    )(bounds, *operands)


def attend_backward(plan, totals, q, out, out_grad, parts, q_offset, fused):
    bounds, interval = plan
    q_array, q_index = q
    n_blocks, columns = interval.shape[1], q_array.shape[2]
    length, groups = n_blocks * BQ, columns // (2 * HD)
    operands = [interval, totals, q_array, out, out_grad]
    specs = [
        whole(interval),
        pl.BlockSpec((1, n_blocks, 2 * BQ), lambda g, *_: (g, 0, 0)),
        column_block(q_array, q_index),
        column_block(out),
        column_block(out_grad),
    ]
    for array, k_index, v_index in parts:
        operands += [array, array]
        specs += [column_block(array, k_index), column_block(array, v_index)]
    n_keys = sum(array.shape[1] for array, *_ in parts)
    if fused:
        out_specs = [pl.BlockSpec((3, n_keys, 2 * HD), lambda g, *_: (0, 0, g))]
        out_shape = [jax.ShapeDtypeStruct((3, n_keys, columns), BF16)]
    else:
        out_specs = [
            pl.BlockSpec((length, 2 * HD), lambda g, *_: (0, g)),
            pl.BlockSpec((2, n_keys, 2 * HD), lambda g, *_: (0, 0, g)),
        ]
        out_shape = [
            jax.ShapeDtypeStruct((length, columns), BF16),
            jax.ShapeDtypeStruct((2, n_keys, columns), BF16),
        ]
    return pl.pallas_call(
        functools.partial(
            backward_kernel, n_parts=len(parts), n_blocks=n_blocks, q_offset=q_offset, fused=fused
        ),
        grid_spec=pltpu.PrefetchScalarGridSpec(
            num_scalar_prefetch=1,
            grid=(groups,),
            in_specs=specs,
            out_specs=out_specs,
            scratch_shapes=[pltpu.VMEM((n_keys, 2 * HD), F32), pltpu.VMEM((n_keys, 2 * HD), F32)],
        ),
        out_shape=out_shape,
        compiler_params=PARAMS,
        cost_estimate=pl.CostEstimate(
            flops=5 * length * n_keys * columns, bytes_accessed=8 * n_keys * columns, transcendentals=length * n_keys
        ),
        name="attend_backward",
    )(bounds, *operands)


def make_plan(starts, ends, bases, n_keys):
    bounds, interval = [], []
    for base in bases:
        first, last = starts - base, ends - base
        interval += [first.reshape(-1, BQ), last.reshape(-1, BQ)]
        low = jnp.clip(first[::BQ] // BK, 0, n_keys // BK)
        high = jnp.clip((last[BQ - 1 :: BQ] + BK - 1) // BK, 0, n_keys // BK)
        bounds.append(jnp.stack([low, high], axis=1).reshape(-1))
    return jnp.concatenate(bounds).astype(jnp.int32), jnp.stack(interval).astype(jnp.int32)


def inverse_rms(rows):
    return lax.rsqrt(jnp.mean(rows * rows, axis=-1, keepdims=True) + EPSILON)


def normalize(rows, gain):
    return rows * inverse_rms(rows) * gain


def normalize_back(rows, gain, cotangent):
    inverse = inverse_rms(rows)
    unit = rows * inverse
    scaled = cotangent * gain
    grad = inverse * (scaled - unit * jnp.mean(scaled * unit, axis=-1, keepdims=True))
    return grad, jnp.sum(cotangent * unit, axis=0)


def gelu_parts(u):
    c = (2.0 / jnp.pi) ** 0.5
    t = jnp.tanh(c * (u + 0.044715 * u * u * u))
    half = 0.5 * (1.0 + t)
    slope = half + 0.5 * u * (1.0 - t * t) * (c * (1.0 + 3.0 * 0.044715 * u * u))
    return u * half, slope


def mm(pattern, a, b):
    return jnp.einsum(pattern, a, b, preferred_element_type=F32)


class Links:
    def __init__(self, n_dp):
        self.n_dp = n_dp
        self.n_bits = n_dp.bit_length() - 1
        self.here = lax.axis_index("dp")

    def bit(self, k):
        return (self.here >> k) & 1

    def across_tp(self, x):
        return lax.ppermute(x, "tp", [(0, 1), (1, 0)])

    def across(self, x, k):
        return lax.ppermute(x, "dp", [(i, i ^ (1 << k)) for i in range(self.n_dp)])

    def merge(self, k, mine, theirs):
        own_first = self.bit(k) == 0
        return jnp.concatenate(
            [jnp.where(own_first, mine, theirs), jnp.where(own_first, theirs, mine)], axis=0
        )

    def part(self, x, index, size):
        return lax.dynamic_slice_in_dim(x, index * size, size, axis=0)

    def fetch(self, shard, bits):
        index = 0
        for place, k in enumerate(bits):
            index = index + (self.bit(k) << place)
        held = self.across_tp(self.part(shard, index, shard.shape[0] >> len(bits)))
        for k in bits:
            held = self.merge(k, held, self.across(held, k))
        return held

    def reduce(self, own, other):
        half = own.shape[0] // 2
        c = self.bit(0)
        sent = jnp.concatenate([self.part(own, 1 - c, half), self.part(other, 1 - c, half)], axis=0)
        got = self.across(sent, 0)
        kept_other = self.add(self.part(other, c, half), got[half:])
        kept = self.add(self.part(own, c, half), got[:half])
        kept = self.add(kept, self.across_tp(kept_other))
        for k in range(1, self.n_bits):
            half = kept.shape[0] // 2
            b = self.bit(k)
            kept = self.add(self.part(kept, b, half), self.across(self.part(kept, 1 - b, half), k))
        for k in reversed(range(self.n_bits)):
            kept = self.merge(k, kept, self.across(kept, k))
        return kept.astype(F32)

    def add(self, a, b):
        return (a.astype(F32) + b.astype(F32)).astype(BF16)

    def total(self, x):
        x = x + self.across_tp(x)
        for k in range(self.n_bits):
            x = x + self.across(x, k)
        return x


def flat(x):
    return x.reshape(-1, x.shape[-1])


def shards(
    n_dp,
    decoder_rows,
    memory_rows,
    output_grad,
    token_segments,
    memory_segments,
    valid_mask,
    norm_gains,
    self_project,
    self_output,
    cross_query,
    cross_memory,
    cross_output,
    gate_up,
    down_weight,
):
    links = Links(n_dp)
    side = lax.axis_index("tp")
    decoder, memory, out_grad = decoder_rows[0], memory_rows[0], output_grad[0]
    tokens, patches, valid = token_segments[0], memory_segments[0], valid_mask[0]
    own_len, features = decoder.shape
    mem_len = memory.shape[0]
    halo = tokens.shape[0] // 4

    halo_rows = lax.ppermute(decoder[-halo:], "tp", [(0, 1)])
    two, three = (1, 0), (2, 1, 0)
    project = (self_project, links.fetch(flat(self_project), two).reshape(self_project.shape))
    out_a = (self_output, links.fetch(self_output, two))
    query_w = (cross_query, links.fetch(cross_query, two))
    memory_w = (cross_memory, links.fetch(flat(cross_memory), two).reshape(cross_memory.shape))
    memory_other = links.across_tp(memory)
    out_c = (cross_output, links.fetch(cross_output, two))
    gate_w = (gate_up, links.fetch(flat(gate_up), three).reshape(gate_up.shape))
    down_w = (down_weight, links.fetch(down_weight, three))
    both = (0, 1)

    own_tokens = lax.dynamic_slice_in_dim(tokens, side * own_len, own_len)
    first_own = side * own_len - halo
    place = jnp.arange(own_len, dtype=jnp.int32)
    starts_a = jnp.sum((tokens[None, :] < own_tokens[:, None]).astype(jnp.int32), axis=1) - first_own
    plan_a = make_plan(starts_a, place + (halo + 1), (0,), own_len + halo)
    starts_c = jnp.sum((patches[None, :] < own_tokens[:, None]).astype(jnp.int32), axis=1)
    ends_c = jnp.sum((patches[None, :] <= own_tokens[:, None]).astype(jnp.int32), axis=1)
    plan_c = make_plan(starts_c, ends_c, (side * mem_len, (1 - side) * mem_len), mem_len)

    resid0 = decoder.astype(F32)
    normed_a = normalize(jnp.concatenate([halo_rows, decoder], axis=0).astype(F32), norm_gains[0]).astype(BF16)
    proj_a = [mm("sd,cdi->csi", normed_a, project[h]).astype(BF16) for h in both]
    att_a, totals_a = zip(
        *[attend_forward(plan_a, (proj_a[h], 0), ((proj_a[h], 1, 2),), halo) for h in both]
    )
    branch_a = mm("si,id->sd", att_a[0], out_a[0]) + mm("si,id->sd", att_a[1], out_a[1])
    resid1 = resid0 + branch_a

    normed_c = normalize(resid1, norm_gains[1]).astype(BF16)
    query_c = [mm("sd,di->si", normed_c, query_w[h]).astype(BF16)[None] for h in both]
    kv_own = [mm("td,cdi->cti", memory, memory_w[h]).astype(BF16) for h in both]
    kv_other = [mm("td,cdi->cti", memory_other, memory_w[h]).astype(BF16) for h in both]
    keys_c = [((kv_own[h], 0, 1), (kv_other[h], 0, 1)) for h in both]
    att_c, totals_c = zip(*[attend_forward(plan_c, (query_c[h], 0), keys_c[h], 0) for h in both])
    branch_c = mm("si,id->sd", att_c[0], out_c[0]) + mm("si,id->sd", att_c[1], out_c[1])
    resid2 = resid1 + branch_c

    normed_m = normalize(resid2, norm_gains[2]).astype(BF16)
    gates = [mm("sd,cdf->csf", normed_m, gate_w[h]) for h in both]
    acts = [gelu_parts(gates[h][0]) for h in both]
    hidden = [(acts[h][0] * gates[h][1]).astype(BF16) for h in both]
    branch_m = mm("sf,fd->sd", hidden[0], down_w[0]) + mm("sf,fd->sd", hidden[1], down_w[1])
    result = resid2 + branch_m

    valid_rows = valid.astype(F32)[:, None]
    grad_m = out_grad.astype(F32) * valid_rows
    full_m = grad_m.astype(BF16)
    hidden_grad = [mm("sd,fd->sf", full_m, down_w[h]) for h in both]
    gate_grads = [
        jnp.stack([hidden_grad[h] * gates[h][1] * acts[h][1], hidden_grad[h] * acts[h][0]]).astype(BF16)
        for h in both
    ]
    ffn_sums = links.reduce(
        *[
            jnp.concatenate(
                [
                    flat(mm("sd,csf->cdf", normed_m, gate_grads[h]).astype(BF16)),
                    mm("sd,sf->df", full_m, hidden[h]).astype(BF16),
                ],
                axis=0,
            )
            for h in both
        ]
    )
    normed_m_grad = mm("csf,cdf->sd", gate_grads[0], gate_w[0]) + mm("csf,cdf->sd", gate_grads[1], gate_w[1])
    resid2_grad, gain_m_grad = normalize_back(resid2, norm_gains[2], normed_m_grad)
    grad_c = grad_m + resid2_grad
    full_c = grad_c.astype(BF16)

    att_c_grad = [mm("sd,id->si", full_c, out_c[h]).astype(BF16) for h in both]
    query_grad, kv_grad = zip(
        *[
            attend_backward(
                plan_c, totals_c[h], (query_c[h], 0), att_c[h], att_c_grad[h], keys_c[h], 0, False
            )
            for h in both
        ]
    )
    memory_partial = mm("cti,cdi->td", kv_grad[0][:, mem_len:], memory_w[0]) + mm(
        "cti,cdi->td", kv_grad[1][:, mem_len:], memory_w[1]
    )
    memory_got = links.across_tp(memory_partial.astype(BF16))
    normed_c_grad = mm("si,di->sd", query_grad[0], query_w[0]) + mm("si,di->sd", query_grad[1], query_w[1])
    memory_all = jnp.concatenate([memory, memory_other], axis=0)
    cross_sums = links.reduce(
        *[
            jnp.concatenate(
                [
                    mm("sd,si->di", full_c, att_c[h]).astype(BF16),
                    mm("sd,si->di", normed_c, query_grad[h]).astype(BF16),
                    flat(mm("td,cti->cdi", memory_all, kv_grad[h]).astype(BF16)),
                ],
                axis=0,
            )
            for h in both
        ]
    )
    resid1_grad, gain_c_grad = normalize_back(resid1, norm_gains[1], normed_c_grad)
    grad_a = grad_c + resid1_grad
    full_a = grad_a.astype(BF16)

    att_a_grad = [mm("sd,id->si", full_a, out_a[h]).astype(BF16) for h in both]
    proj_grad = [
        attend_backward(
            plan_a, totals_a[h], (proj_a[h], 0), att_a[h], att_a_grad[h], ((proj_a[h], 1, 2),), halo, True
        )[0]
        for h in both
    ]
    normed_a_grad = mm("csi,cdi->sd", proj_grad[0], project[0]) + mm("csi,cdi->sd", proj_grad[1], project[1])
    halo_got = lax.ppermute(normed_a_grad[:halo].astype(BF16), "tp", [(1, 0)])
    self_sums = links.reduce(
        *[
            jnp.concatenate(
                [
                    flat(mm("sd,csi->cdi", normed_a, proj_grad[h]).astype(BF16)),
                    mm("sd,si->di", full_a, att_a[h]).astype(BF16),
                ],
                axis=0,
            )
            for h in both
        ]
    )
    normed_a_grad = normed_a_grad[halo:]
    normed_a_grad = jnp.concatenate(
        [normed_a_grad[:-halo], normed_a_grad[-halo:] + halo_got.astype(F32)], axis=0
    )
    resid0_grad, gain_a_grad = normalize_back(resid0, norm_gains[0], normed_a_grad)
    decoder_grad = grad_a + resid0_grad
    memory_grad = (
        mm("cti,cdi->td", kv_grad[0][:, :mem_len], memory_w[0])
        + mm("cti,cdi->td", kv_grad[1][:, :mem_len], memory_w[1])
        + memory_got.astype(F32)
    )

    sums = [jnp.sum(v * v * valid_rows) for v in (result, branch_a, branch_c, branch_m)] + [jnp.sum(valid_rows)]
    stats = jnp.zeros((8, features), F32)
    for row, value in enumerate(sums):
        stats = stats.at[row].set(value)
    stats = links.total(stats.at[5].set(gain_m_grad).at[6].set(gain_c_grad))
    gain_a = links.total(jnp.broadcast_to(gain_a_grad, (8, features)))
    gains_grad = jnp.stack([gain_a[0], stats[6], stats[5]])
    root_squares = jnp.sqrt(stats[:4, 0] / (stats[4, 0] * features))

    d = features
    return (
        result.astype(BF16)[None],
        decoder_grad[None],
        memory_grad[None],
        root_squares,
        gains_grad,
        self_sums[: 3 * d].reshape(self_project.shape),
        self_sums[3 * d :].T,
        cross_sums[d : 2 * d],
        cross_sums[2 * d :].reshape(cross_memory.shape),
        cross_sums[:d].T,
        ffn_sums[: 2 * d].reshape(gate_up.shape),
        ffn_sums[2 * d :].T,
    )


def solution(mesh):
    assert mesh.shape["tp"] == 2
    return jax.shard_map(
        functools.partial(shards, mesh.shape["dp"]),
        mesh=mesh,
        in_specs=(
            P("dp", "tp", None),
            P("dp", "tp", None),
            P("dp", "tp", None),
            P("dp", None),
            P("dp", None),
            P("dp", "tp"),
            P(),
            P(None, None, "tp"),
            P("tp", None),
            P(None, "tp"),
            P(None, None, "tp"),
            P("tp", None),
            P(None, None, "tp"),
            P("tp", None),
        ),
        out_specs=(
            P("dp", "tp", None),
            P("dp", "tp", None),
            P("dp", "tp", None),
            P(),
            P(),
            P(None, None, "tp"),
            P("tp", None),
            P(None, "tp"),
            P(None, None, "tp"),
            P("tp", None),
            P(None, None, "tp"),
            P("tp", None),
        ),
        check_vma=False,
    )
```

```python
import functools
import types

import jax
import jax.numpy as jnp
from jax import lax
from jax.experimental import pallas as pl
from jax.experimental.pallas import tpu as pltpu
from jax.sharding import PartitionSpec as P

HD = 64
EPSILON = 1e-06
NEGATIVE = -1e30
BQ = 128
BK = 256
F32 = jnp.float32
BF16 = jnp.bfloat16


def rows_of_two_heads(block):
    lane = lax.broadcasted_iota(jnp.int32, block.shape, 1)
    zero = jnp.zeros_like(block)
    return jnp.concatenate([jnp.where(lane < HD, block, zero), jnp.where(lane >= HD, block, zero)], axis=0)


def heads_side_by_side(wide):
    return jnp.concatenate([wide[:HD, :BQ], wide[HD:, BQ:]], axis=0).T


def columns_of_two_heads(block):
    turned = block.T
    row = lax.broadcasted_iota(jnp.int32, turned.shape, 0)
    zero = jnp.zeros_like(turned)
    return jnp.concatenate([jnp.where(row < HD, turned, zero), jnp.where(row >= HD, turned, zero)], axis=1)


def twice(row):
    return jnp.concatenate([row, row], axis=1)


def pair(g):
    return slice(2 * HD * g, 2 * HD * (g + 1))


def mask_of(interval_ref, part, b):
    first = interval_ref[2 * part, pl.ds(b, 1), :]
    last = interval_ref[2 * part + 1, pl.ds(b, 1), :]
    return twice(first), twice(last)


def blocks_of(first, last, n_keys):
    low = jnp.min(first.astype(F32)).astype(jnp.int32)
    high = jnp.max(last.astype(F32)).astype(jnp.int32)
    return jnp.clip(low, 0, n_keys) // BK, (jnp.clip(high, 0, n_keys) + BK - 1) // BK


def seen(first, last, j):
    key_iota = lax.broadcasted_iota(jnp.int32, (BK, 2 * BQ), 0)
    return (key_iota >= first - j * BK) & (key_iota < last - j * BK)


def plan_kernel(side_ref, tokens_ref, patches_ref, interval_ref, *, own_len, mem_len, halo):
    side = side_ref[0]
    first_own = side * own_len - halo
    n_blocks = own_len // BQ
    tokens, patches = tokens_ref[...], patches_ref[...]
    tokens_below, patches_below = [], []
    for segment in range(9):
        tokens_below.append(jnp.sum((tokens < segment).astype(F32), axis=1, keepdims=True))
        patches_below.append(jnp.sum((patches < segment).astype(F32), axis=1, keepdims=True))
    for b in range(n_blocks):
        own = tokens_ref[:, pl.ds(pl.multiple_of(side * own_len + b * BQ, BQ), BQ)]
        start_a, start_c, end_c = (jnp.zeros((1, BQ), F32) for _ in range(3))
        for segment in range(8):
            here = own == segment
            start_a = jnp.where(here, tokens_below[segment], start_a)
            start_c = jnp.where(here, patches_below[segment], start_c)
            end_c = jnp.where(here, patches_below[segment + 1], end_c)
        start_a, start_c, end_c = (x.astype(jnp.int32) for x in (start_a, start_c, end_c))
        place = lax.broadcasted_iota(jnp.int32, (1, BQ), 1) + (b * BQ + halo + 1)
        own_base, other_base = side * mem_len, (1 - side) * mem_len
        rows = (
            start_a - first_own,
            place,
            start_c - own_base,
            end_c - own_base,
            start_c - other_base,
            end_c - other_base,
        )
        for i, row in enumerate(rows):
            interval_ref[i, b : b + 1, :] = row


def make_plans(side, tokens, patches, own_len, mem_len, halo):
    intervals = pl.pallas_call(
        functools.partial(plan_kernel, own_len=own_len, mem_len=mem_len, halo=halo),
        grid_spec=pltpu.PrefetchScalarGridSpec(
            num_scalar_prefetch=1,
            grid=(1,),
            in_specs=[whole(tokens.shape), whole(patches.shape)],
            out_specs=whole((6, own_len // BQ, BQ)),
        ),
        out_shape=jax.ShapeDtypeStruct((6, own_len // BQ, BQ), jnp.int32),
        name="key_intervals",
    )(side.reshape(1).astype(jnp.int32), tokens, patches)
    return intervals


def forward_kernel(interval_ref, q_ref, *refs, first_part, n_parts, groups):
    key_refs, (out_ref, total_ref) = refs[: 2 * n_parts], refs[2 * n_parts :]
    b = pl.program_id(0)
    q_wide = []
    for g in range(groups):
        queries = q_ref[:, pair(g)].astype(F32) * (HD**-0.5)
        q_wide.append(columns_of_two_heads(queries).astype(BF16))
    carry = (
        (jnp.full((1, 2 * BQ), NEGATIVE, F32),) * groups,
        (jnp.zeros((1, 2 * BQ), F32),) * groups,
        (jnp.zeros((2 * HD, 2 * BQ), F32),) * groups,
    )
    for part in range(n_parts):
        k_ref, v_ref = key_refs[2 * part], key_refs[2 * part + 1]
        first, last = mask_of(interval_ref, first_part + part, b)
        low, high = blocks_of(first, last, k_ref.shape[0])

        def step(j, carry, k_ref=k_ref, v_ref=v_ref, first=first, last=last):
            rows = pl.ds(pl.multiple_of(j * BK, BK), BK)
            inside = seen(first, last, j)
            peaks, totals, accs = [], [], []
            scores = [
                jnp.where(inside, jnp.dot(k_ref[rows, pair(g)], q_wide[g], preferred_element_type=F32), NEGATIVE)
                for g in range(groups)
            ]
            for g in range(groups):
                peak, total, acc = (c[g] for c in carry)
                new_peak = jnp.maximum(peak, jnp.max(scores[g], axis=0, keepdims=True))
                shrink = jnp.exp(peak - new_peak)
                probs = jnp.exp(scores[g] - new_peak)
                peaks.append(new_peak)
                totals.append(total * shrink + jnp.sum(probs, axis=0, keepdims=True))
                accs.append(
                    acc * shrink
                    + lax.dot_general(
                        v_ref[rows, pair(g)],
                        probs.astype(BF16),
                        (((0,), (0,)), ((), ())),
                        preferred_element_type=F32,
                    )
                )
            return tuple(peaks), tuple(totals), tuple(accs)

        carry = lax.fori_loop(low, high, step, carry)
    for g in range(groups):
        peak, total, acc = (c[g] for c in carry)
        out_ref[:, pair(g)] = heads_side_by_side(acc / total).astype(BF16)
        total_ref[0, g : g + 1, :] = peak + jnp.log(total)


def backward_kernel(
    interval_ref, total_ref, q_ref, out_ref, grad_ref, *refs, first_part, n_parts, n_blocks, groups, q_offset, fused
):
    key_refs, refs = refs[: 2 * n_parts], refs[2 * n_parts :]
    if fused:
        (all_ref, dk_acc, dv_acc) = refs
        columns = all_ref.shape[1] // 3
    else:
        (dq_ref, dkv_ref, dk_acc, dv_acc) = refs
        columns = dq_ref.shape[1]
    b = pl.program_id(0)

    @pl.when(b == 0)
    def _():
        dk_acc[...] = jnp.zeros_like(dk_acc)
        dv_acc[...] = jnp.zeros_like(dv_acc)

    q_rows, q_wide, g_rows, g_wide, inner, log_total = [], [], [], [], [], []
    for g in range(groups):
        queries = q_ref[:, pair(g)].astype(F32) * (HD**-0.5)
        q_rows.append(rows_of_two_heads(queries).astype(BF16))
        q_wide.append(columns_of_two_heads(queries).astype(BF16))
        grad = grad_ref[:, pair(g)].astype(F32)
        g_rows.append(rows_of_two_heads(grad).astype(BF16))
        g_wide.append(columns_of_two_heads(grad).astype(BF16))
        product = (grad * out_ref[:, pair(g)].astype(F32)).T
        inner.append(
            jnp.concatenate(
                [jnp.sum(product[:HD], axis=0, keepdims=True), jnp.sum(product[HD:], axis=0, keepdims=True)], axis=1
            )
        )
        log_total.append(total_ref[0, g : g + 1, :])
    dq = (jnp.zeros((2 * HD, 2 * BQ), F32),) * groups
    base = 0
    for part in range(n_parts):
        k_ref, v_ref = key_refs[2 * part], key_refs[2 * part + 1]
        first, last = mask_of(interval_ref, first_part + part, b)
        low, high = blocks_of(first, last, k_ref.shape[0])

        def step(j, dq, k_ref=k_ref, v_ref=v_ref, first=first, last=last, base=base):
            rows = pl.ds(pl.multiple_of(j * BK, BK), BK)
            sums = pl.ds(pl.multiple_of(base + j * BK, BK), BK)
            inside = seen(first, last, j)
            new = []
            for g in range(groups):
                keys = k_ref[rows, pair(g)]
                scores = jnp.dot(keys, q_wide[g], preferred_element_type=F32)
                prob_grad = jnp.dot(v_ref[rows, pair(g)], g_wide[g], preferred_element_type=F32)
                probs = jnp.exp(jnp.where(inside, scores, NEGATIVE) - log_total[g])
                score_grad = (probs * (prob_grad - inner[g])).astype(BF16)
                dv_acc[sums, pair(g)] += jnp.dot(probs.astype(BF16), g_rows[g], preferred_element_type=F32)
                dk_acc[sums, pair(g)] += jnp.dot(score_grad, q_rows[g], preferred_element_type=F32)
                new.append(
                    dq[g]
                    + lax.dot_general(keys, score_grad, (((0,), (0,)), ((), ())), preferred_element_type=F32)
                )
            return tuple(new)

        dq = lax.fori_loop(low, high, step, dq)
        base += k_ref.shape[0]
    for g in range(groups):
        value = (heads_side_by_side(dq[g]) * (HD**-0.5)).astype(BF16)
        if fused:
            all_ref[pl.ds(pl.multiple_of(q_offset + b * BQ, BQ), BQ), pair(g)] = value
        else:
            dq_ref[:, pair(g)] = value

    @pl.when(b == n_blocks - 1)
    def _():
        if fused:
            if q_offset:
                all_ref[:q_offset, :columns] = jnp.zeros((q_offset, columns), BF16)
            all_ref[:, columns : 2 * columns] = dk_acc[...].astype(BF16)
            all_ref[:, 2 * columns :] = dv_acc[...].astype(BF16)
        else:
            dkv_ref[:, :columns] = dk_acc[...].astype(BF16)
            dkv_ref[:, columns:] = dv_acc[...].astype(BF16)


def row_block(columns, index=0, offset=0):
    return pl.BlockSpec((BQ, columns), lambda b, *_: (b + offset // BQ, index))


def whole(shape):
    return pl.BlockSpec(shape, lambda *_: (0,) * len(shape))


def params(mib):
    return pltpu.CompilerParams(dimension_semantics=("arbitrary",), vmem_limit_bytes=mib << 20)


def attend_forward(intervals, first_part, columns, q, parts, q_offset):
    q_array, q_index = q
    n_blocks = intervals.shape[1]
    length, groups = n_blocks * BQ, columns // (2 * HD)
    operands, specs = [intervals, q_array], [whole(intervals.shape), row_block(columns, q_index, q_offset)]
    for part in parts:
        operands += list(part)
        specs += [whole(x.shape) for x in part]
    return pl.pallas_call(
        functools.partial(forward_kernel, first_part=first_part, n_parts=len(parts), groups=groups),
        grid=(n_blocks,),
        in_specs=specs,
        out_specs=[row_block(columns), pl.BlockSpec((1, groups, 2 * BQ), lambda b: (b, 0, 0))],
        out_shape=[
            jax.ShapeDtypeStruct((length, columns), BF16),
            jax.ShapeDtypeStruct((n_blocks, groups, 2 * BQ), F32),
        ],
        compiler_params=params(14),
        cost_estimate=COST,
        name="attend_forward",
    )(*operands)


def attend_backward(intervals, first_part, columns, totals, q, out, out_grad, parts, q_offset, fused):
    q_array, q_index = q
    n_blocks = intervals.shape[1]
    length, groups = n_blocks * BQ, columns // (2 * HD)
    operands = [intervals, totals, q_array, out, out_grad]
    specs = [
        whole(intervals.shape),
        pl.BlockSpec((1, groups, 2 * BQ), lambda b: (b, 0, 0)),
        row_block(columns, q_index, q_offset),
        row_block(columns),
        row_block(columns),
    ]
    for part in parts:
        operands += list(part)
        specs += [whole(x.shape) for x in part]
    n_keys = sum(keys.shape[0] for keys, _ in parts)
    if fused:
        out_specs = [whole((n_keys, 3 * columns))]
        out_shape = [jax.ShapeDtypeStruct((n_keys, 3 * columns), BF16)]
    else:
        out_specs = [row_block(columns), whole((n_keys, 2 * columns))]
        out_shape = [
            jax.ShapeDtypeStruct((length, columns), BF16),
            jax.ShapeDtypeStruct((n_keys, 2 * columns), BF16),
        ]
    return pl.pallas_call(
        functools.partial(
            backward_kernel,
            first_part=first_part,
            n_parts=len(parts),
            n_blocks=n_blocks,
            groups=groups,
            q_offset=q_offset,
            fused=fused,
        ),
        grid=(n_blocks,),
        in_specs=specs,
        out_specs=out_specs,
        scratch_shapes=[pltpu.VMEM((n_keys, columns), F32), pltpu.VMEM((n_keys, columns), F32)],
        out_shape=out_shape,
        compiler_params=params(18 if fused else 26),
        cost_estimate=COST,
        name="attend_backward",
    )(*operands)


COST = pl.CostEstimate(flops=1 << 20, bytes_accessed=1 << 20, transcendentals=0)


def inverse_rms(rows):
    return lax.rsqrt(jnp.mean(rows * rows, axis=-1, keepdims=True) + EPSILON)


def normalize(rows, gain):
    return rows * inverse_rms(rows) * gain


def normalize_back(rows, gain, cotangent):
    inverse = inverse_rms(rows)
    unit = rows * inverse
    scaled = cotangent * gain
    grad = inverse * (scaled - unit * jnp.mean(scaled * unit, axis=-1, keepdims=True))
    return grad, jnp.sum(cotangent * unit, axis=0)


def gelu_parts(u):
    c = float((2.0 / jnp.pi) ** 0.5)
    t = jnp.tanh(c * (u + 0.044715 * u * u * u))
    half = 0.5 * (1.0 + t)
    slope = half + 0.5 * u * (1.0 - t * t) * (c * (1.0 + 3.0 * 0.044715 * u * u))
    return u * half, slope


def contract(a, b, i, j):
    return lax.dot_general(a, b, (((i,), (j,)), ((), ())), preferred_element_type=F32)


def nn(a, b):
    return contract(a, b, 1, 0)


def nt(a, b):
    return contract(a, b, 1, 1)


def tn(a, b):
    return contract(a, b, 0, 0)


def dot(a, b, i, j):
    return lax.dot_general(a, b, (((i,), (j,)), ((), ())), preferred_element_type=F32)


class Part:
    def __init__(self, array, columns=None, at=0, plane=None, row=0):
        self.array, self.at, self.plane, self.row = array, at, plane, row
        self.columns = array.shape[-1] if columns is None else columns

    def split(self, rows):
        at, row = self.at, self.row // rows
        return pl.BlockSpec((rows, self.columns), lambda i, *_: (row + i, at))

    def spec(self):
        if self.plane is None:
            at = self.at
            return pl.BlockSpec((self.array.shape[0], self.columns), lambda *_: (0, at))
        plane = self.plane
        return pl.BlockSpec((None,) + self.array.shape[1:], lambda *_: (plane, 0, 0))


def back_kernel(*refs, n, m, norm, stacked):
    grads, weights, refs = refs[:n], refs[n : 2 * n], refs[2 * n :]
    total = dot(grads[0][...], weights[0][...], 1, 1)
    for grad, weight in zip(grads[1:], weights[1:]):
        total = total + dot(grad[...], weight[...], 1, 1)
    if not norm:
        add, out_ref = refs[:-1], refs[-1]
        for ref in add:
            total = total + ref[...].astype(F32)
        out_ref[...] = total.astype(out_ref.dtype)
        return
    resid_ref, gain_ref, base_ref = refs[:3]
    out_weights, (grad_ref, full_ref, gain_out), outs = refs[3 : 3 + m], refs[3 + m : 6 + m], refs[6 + m :]
    rows = resid_ref[...]
    inverse = inverse_rms(rows)
    unit = rows * inverse
    scaled = total * gain_ref[...]
    grad = base_ref[...].astype(F32) + inverse * (scaled - unit * jnp.mean(scaled * unit, axis=-1, keepdims=True))
    grad_ref[...] = grad
    full = grad.astype(BF16)
    full_ref[...] = full

    @pl.when(pl.program_id(0) == 0)
    def _():
        gain_out[...] = jnp.zeros_like(gain_out)

    gain_out[...] += jnp.sum(total * unit, axis=0, keepdims=True)
    for weight, out in zip(out_weights, outs):
        out[...] = dot(full, weight[...], 1, 1).astype(BF16)


TILE = 256


def product_back(pairs, length, dtype, add=None):
    n, features = len(pairs), pairs[0][1].array.shape[-2]
    grads, weights = zip(*pairs)
    add = [] if add is None else [add]
    return pl.pallas_call(
        functools.partial(back_kernel, n=n, m=0, norm=False, stacked=0),
        grid=(length // TILE,),
        in_specs=[g.split(TILE) for g in grads] + [w.spec() for w in weights] + [Part(x).split(TILE) for x in add],
        out_specs=pl.BlockSpec((TILE, features), lambda i: (i, 0)),
        out_shape=jax.ShapeDtypeStruct((length, features), dtype),
        compiler_params=params(30),
        cost_estimate=COST,
        name="back",
    )(*[p.array for p in grads], *in_hbm([p.array for p in weights]), *add)


def norm_back(pairs, resid, gain, base, out_weights):
    n, m, (length, features) = len(pairs), len(out_weights), resid.shape
    grads, weights = zip(*pairs)
    tile = lambda x: Part(x).split(TILE)
    widths = [w.shape[0] for w in out_weights]
    return pl.pallas_call(
        functools.partial(back_kernel, n=n, m=m, norm=True, stacked=0),
        grid=(length // TILE,),
        in_specs=[g.split(TILE) for g in grads]
        + [w.spec() for w in weights]
        + [tile(resid), whole((1, features)), tile(base)]
        + [whole(w.shape) for w in out_weights],
        out_specs=[pl.BlockSpec((TILE, features), lambda i: (i, 0))] * 2
        + [whole((1, features))]
        + [pl.BlockSpec((TILE, w), lambda i: (i, 0)) for w in widths],
        out_shape=[
            jax.ShapeDtypeStruct((length, features), F32),
            jax.ShapeDtypeStruct((length, features), BF16),
            jax.ShapeDtypeStruct((1, features), F32),
        ]
        + [jax.ShapeDtypeStruct((length, w), BF16) for w in widths],
        compiler_params=params(34),
        cost_estimate=COST,
        name="norm_back",
    )(*[p.array for p in grads], *[p.array for p in weights], resid, gain.reshape(1, -1), base, *out_weights)


def weight_kernel(*refs, n, m):
    rows, grads, outs, turned = refs[:n], refs[n : n + m], refs[n + m : n + 2 * m], refs[-1]

    @pl.when(pl.program_id(0) == 0)
    def _():
        at = 0
        for ref in rows:
            for first in range(0, ref.shape[0], TILE):
                turned[:, at + first : at + first + TILE] = ref[first : first + TILE, :].astype(F32).T.astype(BF16)
            at += ref.shape[0]

    for grad, out in zip(grads, outs):
        out[...] = dot(turned[...], grad[...], 1, 0).astype(BF16)


def weight_grads(rows, grads, chunk):
    length, features = sum(x.shape[0] for x in rows), rows[0].shape[1]
    columns = grads[0].shape[1]
    return pl.pallas_call(
        functools.partial(weight_kernel, n=len(rows), m=len(grads)),
        grid=(columns // chunk,),
        in_specs=[whole(x.shape) for x in rows]
        + [pl.BlockSpec((length, chunk), lambda j: (0, j)) for _ in grads],
        out_specs=[pl.BlockSpec((features, chunk), lambda j: (0, j)) for _ in grads],
        out_shape=[jax.ShapeDtypeStruct((features, columns), BF16) for _ in grads],
        scratch_shapes=[pltpu.VMEM((features, length), BF16)],
        compiler_params=params(30),
        cost_estimate=COST,
        name="weight_grads",
    )(*rows, *grads)


def ffn_kernel(normed_ref, full_ref, gate_ref, up_ref, down_ref, hidden_ref, grads_ref, *, chunk, units):
    j = pl.program_id(0)
    gate = dot(normed_ref[...], gate_ref[...], 1, 0)
    up = dot(normed_ref[...], up_ref[...], 1, 0)
    hidden_grad = dot(full_ref[...], down_ref[...], 1, 1)
    act, slope = gelu_parts(gate)
    hidden_ref[...] = (act * up).astype(BF16)
    at = pl.multiple_of(j * chunk, chunk)
    grads_ref[:, pl.ds(at, chunk)] = (hidden_grad * up * slope).astype(BF16)
    grads_ref[:, pl.ds(pl.multiple_of(units + at, chunk), chunk)] = (hidden_grad * act).astype(BF16)


def feed_forward(normed, full, gate, up, down, chunk=256):
    (length, features), units = normed.shape, down.shape[0]

    def columns(part):
        if part.plane is None:
            first = part.at * part.columns // chunk
            return pl.BlockSpec((features, chunk), lambda j: (0, first + j))
        plane = part.plane
        return pl.BlockSpec((None, features, chunk), lambda j: (plane, 0, j))

    return pl.pallas_call(
        functools.partial(ffn_kernel, chunk=chunk, units=units),
        grid=(units // chunk,),
        in_specs=[
            whole(normed.shape),
            whole(full.shape),
            columns(gate),
            columns(up),
            pl.BlockSpec((chunk, features), lambda j: (j, 0)),
        ],
        out_specs=[pl.BlockSpec((length, chunk), lambda j: (0, j)), whole((length, 2 * units))],
        out_shape=[
            jax.ShapeDtypeStruct((length, units), BF16),
            jax.ShapeDtypeStruct((length, 2 * units), BF16),
        ],
        compiler_params=params(24),
        cost_estimate=COST,
        name="feed_forward",
    )(normed, full, *in_hbm([gate.array, up.array, down]))


def in_hbm(arrays):
    return [pltpu.with_memory_space_constraint(x, pltpu.HBM) for x in arrays]


def tie(x, *others):
    return lax.optimization_barrier((x, others))[0] if others else x


def arrange_kernel(scalars, mine_ref, theirs_ref, *out_refs, outputs):
    top = scalars[1]
    at = 0
    for out_ref, (width, planes) in zip(out_refs, outputs):
        for plane in range(max(planes, 1)):
            mine, theirs = (ref[0, :, at : at + width].astype(out_ref.dtype) for ref in (mine_ref, theirs_ref))
            at += width
            if planes:
                out_ref[plane, top, 0] = mine
                out_ref[plane, 1 - top, 0] = theirs
            else:
                out_ref[0, :, :width] = jnp.where(top == 0, mine, theirs)
                out_ref[0, :, width:] = jnp.where(top == 0, theirs, mine)


def arrange(mine, theirs, index, top, outputs, dtype):
    n, rows, columns = mine.shape
    scalars = jnp.stack([index, top]).astype(jnp.int32)
    specs, shapes = [], []
    for w, planes in outputs:
        if planes:
            specs.append(pl.BlockSpec((planes, 2, 1, rows, w), lambda i, sc: (0, 0, i, 0, 0)))
            shapes.append(jax.ShapeDtypeStruct((planes, 2, n, rows, w), dtype))
        else:
            specs.append(pl.BlockSpec((1, rows, 2 * w), lambda i, sc: (i, 0, 0)))
            shapes.append(jax.ShapeDtypeStruct((n, rows, 2 * w), dtype))
    outs = pl.pallas_call(
        functools.partial(arrange_kernel, outputs=outputs),
        grid_spec=pltpu.PrefetchScalarGridSpec(
            num_scalar_prefetch=1,
            grid=(n,),
            in_specs=[pl.BlockSpec((1, rows, columns), lambda i, sc: (i ^ sc[0], 0, 0))] * 2,
            out_specs=specs,
        ),
        out_shape=shapes,
        compiler_params=params(12),
        cost_estimate=COST,
        name="arrange",
    )(scalars, mine, theirs)
    return [
        x.reshape(x.shape[0], 2 * n * rows, w) if planes else x.reshape(n * rows, 2 * w)
        for x, (w, planes) in zip(outs, outputs)
    ]


class Links:
    def __init__(self, n_dp):
        self.n_dp = n_dp
        self.n_bits = n_dp.bit_length() - 1
        self.here = lax.axis_index("dp")

    def bit(self, k):
        return (self.here >> k) & 1

    def across_tp(self, x):
        return lax.ppermute(x, "tp", [(0, 1), (1, 0)])

    def across(self, x, mask):
        return lax.ppermute(x, "dp", [(i, i ^ mask) for i in range(self.n_dp)])


class Single:
    def __init__(self, move):
        self.move, self.started = move, False

    def send(self, x, *after):
        self.sent = tie(x, *after)
        self.got = [self.move(self.sent)]

    def take(self):
        return self.got[0]


class Fetch:
    def __init__(self, links, shards, bits, outputs):
        self.links, self.bits, self.outputs = links, list(bits), outputs
        self.n, self.index, self.got, self.held = 1 << len(bits), 0, None, None
        for place, k in enumerate(bits):
            self.index = self.index + (links.bit(k) << place)
        self.piece = jnp.concatenate([y for x in shards for y in self.pieces(x)], axis=2)

    def pieces(self, x):
        if isinstance(x, tuple):
            (x,) = x
            rows, columns, half = x.shape[0] * 2 // self.n, x.shape[1] // 2, self.n // 2
            at = (self.index % half * rows, self.index // half * columns)
            return [lax.dynamic_slice(x, at, (rows, columns))[None]]
        x = x.reshape(-1, self.n, x.shape[-2] // self.n, x.shape[-1])
        return list(lax.dynamic_slice_in_dim(x, self.index, 1, axis=1))

    def send(self, *after):
        if self.held is None:
            self.sent = tie(self.piece, *after)
            self.got = [self.links.across_tp(self.sent)]
        else:
            self.sent = tie(self.held, *after)
            self.got = [self.links.across(self.sent, 1 << self.bits[0])]

    def take(self):
        if self.held is None:
            self.held = self.got[0]
            return
        self.bits.pop(0)
        if self.bits:
            self.held = jnp.concatenate([self.held, self.got[0]], axis=0)
            if len(self.bits) == 1:
                self.last = self.bits[0]
        else:
            self.theirs = self.got[0]

    def ended(self):
        return not self.bits

    def finish(self):
        top, below = self.links.bit(self.last), self.index & (self.n // 2 - 1)
        whole_arrays = arrange(self.held, self.theirs, below, top, self.outputs, BF16)
        return [x[0] if x.ndim == 3 and x.shape[0] == 1 else x for x in whole_arrays]


TP = "tp"
HALO, PROJECT, MEMORY, GATE, DOWN, REST, CROSS, SELF = range(8)


class Reduction:
    def __init__(self, links, own, other, order, outputs):
        self.links, self.order, self.outputs = links, list(order), outputs
        self.back = [k for k in reversed(order) if k is not TP][:-1]
        self.n_blocks = links.n_dp
        view = lambda x: x.reshape(self.n_blocks, -1, x.shape[-1])
        self.own, self.other = [([view(x) for x in own], 0)], [([view(x) for x in other], 0)]
        self.at, self.size = 0, self.n_blocks
        self.index = 0
        self.result = self.theirs = None

    def piece(self, addends, at, size):
        total = 0.0
        for arrays, base in addends:
            parts = [lax.dynamic_slice_in_dim(x, at - base, size).astype(F32) for x in arrays]
            total = total + (jnp.concatenate(parts, axis=2) if len(parts) > 1 else parts[0])
        return total.astype(BF16)

    def send(self, *after):
        links = self.links
        if self.result is not None:
            bits = self.back[0] if self.back else (0,)
            masks = self.masks(bits)
            self.sent = tie(self.result, *after)
            self.got = [links.across(self.sent, mask) for mask in masks]
        elif self.order[0] is TP:
            self.sent = tie(self.piece(self.other, self.at, self.size), *after)
            self.got = [links.across_tp(self.sent)]
            self.other = None
        else:
            bits = self.order[0]
            masks = self.masks(bits)
            digit = 0
            for k in bits:
                digit = digit * 2 + links.bit(k)
            part = self.size // (len(masks) + 1)
            self.got, self.sent = [], []
            for i, mask in enumerate(masks):
                at = self.at + (digit ^ (i + 1)) * part
                sent = self.piece(self.own, at, part)
                if self.other is not None:
                    sent = jnp.concatenate([sent, self.piece(self.other, at, part)], axis=0)
                self.sent.append(tie(sent, *after))
                self.got.append(links.across(self.sent[-1], mask))
            self.at, self.size = self.at + digit * part, part
            if bits != (0,):
                self.index = self.index * (len(masks) + 1) + digit
        return self.got

    def masks(self, bits):
        out = []
        for i in range(1, 1 << len(bits)):
            out.append(sum(1 << k for place, k in enumerate(reversed(bits)) if (i >> place) & 1))
        return out

    def take(self):
        if self.result is not None:
            if self.back:
                self.back.pop(0)
                self.result = jnp.concatenate([self.result] + self.got, axis=0)
            else:
                self.theirs = self.got[0]
            return self.result
        self.order.pop(0)
        for got in self.got:
            self.own = self.own + [([got[: self.size]], self.at)]
            if self.other is not None:
                self.other = self.other + [([got[self.size :]], self.at)]
        if not self.order:
            self.result = self.piece(self.own, self.at, self.size)
        return self.got

    def ended(self):
        return self.theirs is not None

    def finish(self):
        return arrange(self.result, self.theirs, self.index, self.links.bit(0), self.outputs, F32)


class Agenda:
    def __init__(self, links):
        self.links, self.chains, self.now, self.strict = links, {}, (), True

    def at(self, x):
        return tie(x, *self.now)

    def after(self, *values):
        self.now = values

    def start(self, name, chain, *args):
        self.chains[name] = chain
        chain.send(*args, *self.now)
        self.now = (self.now, chain.sent)

    def go(self, name):
        chain = self.chains[name]
        if self.strict:
            chain.got = tie(chain.got, *self.now)
        came = chain.got
        chain.take()
        if chain.ended():
            self.now = (came,)
            return chain.finish()
        chain.send(came, *self.now)
        self.now = (came, chain.sent)

    def take(self, name):
        came = self.chains[name].take()
        if self.strict:
            came = tie(came, *self.now)
        self.now = (self.now, came)
        return came


def column_halves(x):
    half = x.shape[1] // 2
    return jnp.concatenate([x[:, :half], x[:, half:]], axis=0)


def beside(x):
    return jnp.concatenate(list(x), axis=1)


def shards(
    n_dp,
    decoder_rows,
    memory_rows,
    output_grad,
    token_segments,
    memory_segments,
    valid_mask,
    norm_gains,
    self_project,
    self_output,
    cross_query,
    cross_memory,
    cross_output,
    gate_up,
    down_weight,
):
    links = Links(n_dp)
    side = lax.axis_index("tp")
    decoder, memory, out_grad = decoder_rows[0], memory_rows[0], output_grad[0]
    valid = valid_mask[0]
    own_len, features = decoder.shape
    mem_len, columns = memory.shape[0], cross_query.shape[1]
    halo = token_segments.shape[1] // 4
    both = (0, 1)

    d, units = features, down_weight.shape[0]
    half_len = mem_len // 2
    agenda = Agenda(links)
    at, after, start, go, take = agenda.at, agenda.after, agenda.start, agenda.go, agenda.take
    v = types.SimpleNamespace()
    v.kv_own_of = [None, None]
    v.self_of = [None, None]
    v.cross_of = [None, None]
    v.query_grad_of = [None, None]
    v.kv_grad_of = [None, None]
    v.memory_dw_of = [None, None]
    v.proj_grad_of = [None, None]
    v.memory_came, v.memory_got = [], []
    bit0, bit1, rest = (0,), (1,), [(k,) for k in range(2, links.n_bits)]
    tp_first, tp_second, tp_third = (
        [bit0, TP, bit1] + rest,
        [bit0, bit1, TP] + rest,
        [bit0, bit1] + rest[:1] + [TP] + rest[1:],
    )
    resid0 = decoder.astype(F32)
    valid_rows = valid.astype(F32)[:, None]
    grad_m = out_grad.astype(F32) * valid_rows
    full_m = grad_m.astype(BF16)

    def sums(name, order, outputs, parts):
        after(parts)
        start(name, Reduction(links, *parts, order, outputs))

    def send_halo():
        start(HALO, Single(lambda x: lax.ppermute(x, "tp", [(0, 1)])), decoder[-halo:])

    def send_project():
        start(PROJECT, Fetch(links, [self_project], BITS, ((columns, 3),)))

    def send_memory(i):
        start(MEMORY, Single(links.across_tp), memory)

    def send_ffn():
        def mine(x):
            blocks = x.reshape(-1, links.n_dp, x.shape[-2] // links.n_dp, x.shape[-1])
            return jnp.concatenate(list(lax.dynamic_index_in_dim(blocks, links.here, 1, False)), axis=1)

        start(GATE, Single(links.across_tp), mine(gate_up))
        start(DOWN, Single(links.across_tp), mine(down_weight))

    def gather_ffn():
        gate_other = lax.all_gather(take(GATE), "dp", axis=0, tiled=True)
        v.gate_w = [Part(gate_up, plane=c) for c in both], [Part(gate_other, units, c) for c in both]
        v.down_w = (down_weight, lax.all_gather(take(DOWN), "dp", axis=0, tiled=True))

    def send_rest():
        start(
            REST,
            Fetch(
                links,
                [cross_memory, cross_query, (self_output,), (cross_output,)],
                BITS,
                ((columns, 2), (columns, 1), (columns, 0), (columns, 0)),
            ),
        )

    def plan():
        v.intervals = make_plans(side, token_segments, memory_segments, own_len, mem_len, halo)
        after(v.intervals)

    def norm_a():
        v.rows_a = jnp.concatenate([take(HALO), decoder], axis=0).astype(F32)
        v.normed_a = normalize(v.rows_a, norm_gains[0]).astype(BF16)

    def self_forward(h):
        if h:
            v.project = (self_project, out[PROJECT][0])
        weights = v.project[1] if h else self_project
        rows = at(v.normed_a)
        proj = [nn(rows, weights[c]).astype(BF16) for c in range(3)]
        att, totals = attend_forward(v.intervals, 0, columns, (proj[0], 0), ((proj[1], proj[2]),), halo)
        v.self_of[h] = proj, att, totals
        after(att)

    def keys_of(rows, h):
        return tuple(nn(rows, v.memory_w[h][c]).astype(BF16) for c in both)

    def keys_own(h):
        v.kv_own_of[h] = keys_of(at(memory), h)
        after(v.kv_own_of[h])

    def weights_rest():
        other_memory, other_query, other_out_a, other_out_c = out[REST]
        v.memory_w = (cross_memory, other_memory)
        v.out_a, v.out_c, v.query_w = (
            (self_output, other_out_a),
            (cross_output, other_out_c),
            (cross_query, other_query),
        )

    def queries():
        weights_rest()
        v.proj_a, v.att_a, v.totals_a = zip(*v.self_of)
        att = at(v.att_a)
        v.branch_a = nn(att[0], v.out_a[0]) + nn(att[1], v.out_a[1])
        v.resid1 = resid0 + v.branch_a
        v.normed_c = normalize(v.resid1, norm_gains[1]).astype(BF16)
        v.query_c = [nn(v.normed_c, v.query_w[h]).astype(BF16) for h in both]
        after(v.query_c)

    def take_memory():
        v.memory_came.append(take(MEMORY))

    def cross_forward(h):
        if not h:
            (v.memory_other,) = v.memory_came
        keys = (v.kv_own_of[h], keys_of(at(v.memory_other), h))
        att, totals = attend_forward(v.intervals, 1, columns, (v.query_c[h], 0), keys, 0)
        v.cross_of[h] = keys, att, totals
        after(att)

    def ffn():
        v.keys_c, v.att_c, v.totals_c = zip(*v.cross_of)
        att = at(v.att_c)
        v.branch_c = nn(att[0], v.out_c[0]) + nn(att[1], v.out_c[1])
        v.resid2 = v.resid1 + v.branch_c
        v.normed_m = normalize(v.resid2, norm_gains[2]).astype(BF16)
        v.hidden, v.gate_grads = zip(
            *[feed_forward(v.normed_m, full_m, *v.gate_w[h], v.down_w[h]) for h in both]
        )
        after(v.gate_grads)

    def gate_dw():
        agenda.strict = False
        parts = weight_grads([v.normed_m], at(list(v.gate_grads)), 512)
        sums(GATE, ORDERS[GATE], ((units, 2),), [[x] for x in parts])

    def down_dw():
        v.down_dw = weight_grads([at(full_m)], list(v.hidden), 512)
        after(v.down_dw)

    def norm_m_grad():
        v.gate_late = at(v.gate_grads)

    def norm_m_back():
        pairs = [(Part(v.gate_late[h], units, c), v.gate_w[h][c]) for h in both for c in both]
        v.grad_c, v.full_c, gain, *v.att_c_grad = norm_back(pairs, v.resid2, norm_gains[2], full_m, v.out_c)
        v.gain_m = gain[0]
        after(v.att_c_grad)

    def outs_dw():
        grad = at(v.full_c)
        out_dw = [weight_grads([v.att_c[h]], [grad], grad.shape[1])[0] for h in both]
        parts = [[v.down_dw[h], column_halves(out_dw[h])] for h in both]
        sums(DOWN, ORDERS[DOWN], ((units, 1), (columns, 0)), parts)

    def cross_backward(h):
        grad = at(v.att_c_grad[h])
        query = (v.query_c[h], 0)
        v.query_grad_of[h], v.kv_grad_of[h] = attend_backward(
            v.intervals, 1, columns, v.totals_c[h], query, v.att_c[h], grad, v.keys_c[h], 0, False
        )
        after(v.query_grad_of[h])

    def norm_c_back():
        grads = at(v.query_grad_of)
        pairs = [(Part(grads[h]), Part(v.query_w[h])) for h in both]
        v.grad_a, v.full_a, gain, *v.att_a_grad = norm_back(pairs, v.resid1, norm_gains[1], v.grad_c, v.out_a)
        v.gain_c = gain[0]
        after(v.att_a_grad)

    def memory_back(own):
        kv = at(v.kv_grad_of)
        row = 0 if own else mem_len
        pairs = [(Part(kv[h], columns, c, row=row), Part(v.memory_w[h], plane=c)) for h in both for c in both]
        if own:
            v.memory_grad = product_back(pairs, mem_len, F32, v.memory_got[0])
            after(v.memory_grad)
        else:
            v.memory_partial = product_back(pairs, mem_len, BF16)
            after(v.memory_partial)

    def send_partial(i):
        start(MEMORY, Single(links.across_tp), v.memory_partial)

    def take_partial():
        v.memory_got.append(take(MEMORY))

    def memory_dw(h):
        if h:
            v.memory_dw_of = weight_grads([memory, v.memory_other], at(v.kv_grad_of), 384)
            after(v.memory_dw_of)

    def cross_dw():
        query_dw = weight_grads([at(v.normed_c)], v.query_grad_of, columns)
        out_dw = [weight_grads([v.att_a[h]], [at(v.full_a)], v.full_a.shape[1])[0] for h in both]
        parts = [[v.memory_dw_of[h], query_dw[h], column_halves(out_dw[h])] for h in both]
        sums(CROSS, ORDERS[CROSS], ((columns, 2), (columns, 1), (columns, 0)), parts)

    def self_backward(h):
        grad = at(v.att_a_grad[h])
        proj, *keys = v.proj_a[h]
        v.proj_grad_of[h] = attend_backward(
            v.intervals, 0, columns, v.totals_a[h], (proj, 0), v.att_a[h], grad, (keys,), halo, True
        )[0]
        after(v.proj_grad_of[h])

    def norm_a_grad():
        grads = at(v.proj_grad_of)
        pairs = [(Part(grads[h], columns, c), Part(v.project[h], plane=c)) for h in both for c in range(3)]
        v.normed_a_grad = total = product_back(pairs, own_len + halo, F32)
        after(total)
        start(HALO, Single(lambda x: lax.ppermute(x, "tp", [(1, 0)])), total[:halo].astype(BF16))
        v.branch_m = nn(v.hidden[0], v.down_w[0]) + nn(v.hidden[1], v.down_w[1])
        v.result = v.resid2 + v.branch_m
        gain_a = jnp.sum(total * v.rows_a * inverse_rms(v.rows_a), axis=0)
        rows = [jnp.sum(x * x * valid_rows, axis=0) for x in (v.result, v.branch_a, v.branch_c, v.branch_m)]
        rows += [jnp.sum(jnp.broadcast_to(valid_rows, resid0.shape), axis=0), v.gain_m, v.gain_c, gain_a]
        v.stats = jnp.pad(jnp.stack(rows), ((0, 2 * HD - len(rows)), (0, 0))).T.astype(BF16)

    def self_dw():
        parts = [[x, v.stats] for x in weight_grads([v.normed_a], at(v.proj_grad_of), 384)]
        sums(SELF, ORDERS[SELF], ((columns, 3), (2 * HD, 1)), parts)

    def norm_a_back():
        came = take(HALO).astype(F32)
        own = at(v.normed_a_grad[halo:])
        own = jnp.concatenate([own[:-halo], own[-halo:] + came], axis=0)
        resid0_grad, _ = normalize_back(resid0, norm_gains[0], own)
        v.decoder_grad = v.grad_a + resid0_grad
        after(v.decoder_grad)

    BITS = (2, 1, 0)
    ORDERS = {GATE: tp_first, DOWN: tp_second, CROSS: tp_second, SELF: tp_first}
    v.memory_w = (None, None)
    out = {}

    def keys_first():
        v.memory_w = (cross_memory, None)
        keys_own(0)

    def advance(name):
        came = go(name)
        if came is not None:
            out[name] = came
            after(came)

    def for_each(block):
        return [functools.partial(block, h) for h in both]

    mem0, mem1 = for_each(send_memory)
    self0, self1 = for_each(self_forward)
    keys0, keys1 = keys_first, functools.partial(keys_own, 1)
    cross0, cross1 = for_each(cross_forward)
    cross_b0, cross_b1 = for_each(cross_backward)
    part0, part1 = for_each(send_partial)
    mem_dw0, mem_dw1 = for_each(memory_dw)
    self_b0, self_b1 = for_each(self_backward)
    mem_b0, mem_b1 = for_each(memory_back)
    P_, R, A, B, E, D = [functools.partial(advance, name) for name in (PROJECT, REST, GATE, DOWN, CROSS, SELF)]
    agenda_steps = (
        send_halo, send_project, send_ffn, plan, norm_a, P_, gather_ffn, send_rest, self0, P_, mem0, R, keys0, P_, R,
        P_, self1, take_memory, R, R, queries, keys1, cross0, cross1, ffn, gate_dw, down_dw, norm_m_grad, A,
        norm_m_back, outs_dw, cross_b0, B, cross_b1, A, norm_c_back, mem_b0, part0, B, mem_dw0, mem_dw1, cross_dw, A,
        B, self_b1, E, A, B, self_b0, A, B, norm_a_grad, self_dw, E, A, B, take_partial, D, mem_b1, A, B, norm_a_back,
        E, D, A, B, E, D, A, E, D, B, E, D, E, D, E, D, E, D, D,
    )
    for step in agenda_steps:
        step()
    for name in (GATE, DOWN, CROSS, SELF):
        while name not in out:
            advance(name)

    stats = out[SELF][1][0, :, :8].T
    gains_grad = jnp.stack([stats[7], stats[6], stats[5]])
    root_squares = jnp.sqrt(jnp.sum(stats[:4], axis=1) / jnp.sum(stats[4]))
    return (
        v.result.astype(BF16)[None],
        v.decoder_grad[None],
        v.memory_grad[None],
        root_squares,
        gains_grad,
        out[SELF][0],
        out[CROSS][2],
        out[CROSS][1][0],
        out[CROSS][0],
        out[DOWN][1],
        out[GATE][0],
        out[DOWN][0][0].T,
    )


def solution(mesh):
    assert mesh.shape["tp"] == 2
    return jax.shard_map(
        functools.partial(shards, mesh.shape["dp"]),
        mesh=mesh,
        in_specs=(
            P("dp", "tp", None),
            P("dp", "tp", None),
            P("dp", "tp", None),
            P("dp", None),
            P("dp", None),
            P("dp", "tp"),
            P(),
            P(None, None, "tp"),
            P("tp", None),
            P(None, "tp"),
            P(None, None, "tp"),
            P("tp", None),
            P(None, None, "tp"),
            P("tp", None),
        ),
        out_specs=(
            P("dp", "tp", None),
            P("dp", "tp", None),
            P("dp", "tp", None),
            P(),
            P(),
            P(None, None, "tp"),
            P("tp", None),
            P(None, "tp"),
            P(None, None, "tp"),
            P("tp", None),
            P(None, None, "tp"),
            P("tp", None),
        ),
        check_vma=False,
    )
```

```python
import functools
import types

import jax
import jax.numpy as jnp
from jax import lax
from jax.experimental import pallas as pl
from jax.experimental.pallas import tpu as pltpu
from jax.sharding import PartitionSpec as P

HD = 64
EPSILON = 1e-06
NEGATIVE = -1e30
BQ = 128
BK = 256
F32 = jnp.float32
BF16 = jnp.bfloat16


def rows_of_two_heads(block):
    lane = lax.broadcasted_iota(jnp.int32, block.shape, 1)
    zero = jnp.zeros_like(block)
    return jnp.concatenate([jnp.where(lane < HD, block, zero), jnp.where(lane >= HD, block, zero)], axis=0)


def heads_side_by_side(wide):
    return jnp.concatenate([wide[:HD, :BQ], wide[HD:, BQ:]], axis=0).T


def columns_of_two_heads(block):
    turned = block.T
    row = lax.broadcasted_iota(jnp.int32, turned.shape, 0)
    zero = jnp.zeros_like(turned)
    return jnp.concatenate([jnp.where(row < HD, turned, zero), jnp.where(row >= HD, turned, zero)], axis=1)


def twice(row):
    return jnp.concatenate([row, row], axis=1)


def pair(g):
    return slice(2 * HD * g, 2 * HD * (g + 1))


def mask_of(interval_ref, part, b):
    first = interval_ref[2 * part, pl.ds(b, 1), :]
    last = interval_ref[2 * part + 1, pl.ds(b, 1), :]
    return twice(first), twice(last)


def blocks_of(first, last, n_keys):
    low = jnp.min(first.astype(F32)).astype(jnp.int32)
    high = jnp.max(last.astype(F32)).astype(jnp.int32)
    return jnp.clip(low, 0, n_keys) // BK, (jnp.clip(high, 0, n_keys) + BK - 1) // BK


def seen(first, last, j):
    key_iota = lax.broadcasted_iota(jnp.int32, (BK, 2 * BQ), 0)
    return (key_iota >= first - j * BK) & (key_iota < last - j * BK)


def plan_kernel(side_ref, tokens_ref, patches_ref, interval_ref, *, own_len, mem_len, halo):
    side = side_ref[0]
    first_own = side * own_len - halo
    n_blocks = own_len // BQ
    tokens, patches = tokens_ref[...], patches_ref[...]
    tokens_below, patches_below = [], []
    for segment in range(9):
        tokens_below.append(jnp.sum((tokens < segment).astype(F32), axis=1, keepdims=True))
        patches_below.append(jnp.sum((patches < segment).astype(F32), axis=1, keepdims=True))
    for b in range(n_blocks):
        own = tokens_ref[:, pl.ds(pl.multiple_of(side * own_len + b * BQ, BQ), BQ)]
        start_a, start_c, end_c = (jnp.zeros((1, BQ), F32) for _ in range(3))
        for segment in range(8):
            here = own == segment
            start_a = jnp.where(here, tokens_below[segment], start_a)
            start_c = jnp.where(here, patches_below[segment], start_c)
            end_c = jnp.where(here, patches_below[segment + 1], end_c)
        start_a, start_c, end_c = (x.astype(jnp.int32) for x in (start_a, start_c, end_c))
        place = lax.broadcasted_iota(jnp.int32, (1, BQ), 1) + (b * BQ + halo + 1)
        own_base, other_base = side * mem_len, (1 - side) * mem_len
        rows = (
            start_a - first_own,
            place,
            start_c - own_base,
            end_c - own_base,
            start_c - other_base,
            end_c - other_base,
        )
        for i, row in enumerate(rows):
            interval_ref[i, b : b + 1, :] = row


def make_plans(side, tokens, patches, own_len, mem_len, halo):
    intervals = pl.pallas_call(
        functools.partial(plan_kernel, own_len=own_len, mem_len=mem_len, halo=halo),
        grid_spec=pltpu.PrefetchScalarGridSpec(
            num_scalar_prefetch=1,
            grid=(1,),
            in_specs=[whole(tokens.shape), whole(patches.shape)],
            out_specs=whole((6, own_len // BQ, BQ)),
        ),
        out_shape=jax.ShapeDtypeStruct((6, own_len // BQ, BQ), jnp.int32),
        name="key_intervals",
    )(side.reshape(1).astype(jnp.int32), tokens, patches)
    return intervals


def forward_kernel(interval_ref, q_ref, *refs, first_part, n_parts, groups):
    key_refs, (out_ref, total_ref) = refs[: 2 * n_parts], refs[2 * n_parts :]
    b = pl.program_id(0)
    q_wide = []
    for g in range(groups):
        queries = q_ref[:, pair(g)].astype(F32) * (HD**-0.5)
        q_wide.append(columns_of_two_heads(queries).astype(BF16))
    carry = (
        (jnp.full((1, 2 * BQ), NEGATIVE, F32),) * groups,
        (jnp.zeros((1, 2 * BQ), F32),) * groups,
        (jnp.zeros((2 * HD, 2 * BQ), F32),) * groups,
    )
    for part in range(n_parts):
        k_ref, v_ref = key_refs[2 * part], key_refs[2 * part + 1]
        first, last = mask_of(interval_ref, first_part + part, b)
        low, high = blocks_of(first, last, k_ref.shape[0])

        def step(j, carry, k_ref=k_ref, v_ref=v_ref, first=first, last=last):
            rows = pl.ds(pl.multiple_of(j * BK, BK), BK)
            inside = seen(first, last, j)
            peaks, totals, accs = [], [], []
            scores = [
                jnp.where(inside, jnp.dot(k_ref[rows, pair(g)], q_wide[g], preferred_element_type=F32), NEGATIVE)
                for g in range(groups)
            ]
            for g in range(groups):
                peak, total, acc = (c[g] for c in carry)
                new_peak = jnp.maximum(peak, jnp.max(scores[g], axis=0, keepdims=True))
                shrink = jnp.exp(peak - new_peak)
                probs = jnp.exp(scores[g] - new_peak)
                peaks.append(new_peak)
                totals.append(total * shrink + jnp.sum(probs, axis=0, keepdims=True))
                accs.append(
                    acc * shrink
                    + lax.dot_general(
                        v_ref[rows, pair(g)],
                        probs.astype(BF16),
                        (((0,), (0,)), ((), ())),
                        preferred_element_type=F32,
                    )
                )
            return tuple(peaks), tuple(totals), tuple(accs)

        carry = lax.fori_loop(low, high, step, carry)
    for g in range(groups):
        peak, total, acc = (c[g] for c in carry)
        out_ref[:, pair(g)] = heads_side_by_side(acc / total).astype(BF16)
        total_ref[0, g : g + 1, :] = peak + jnp.log(total)


def backward_kernel(
    interval_ref, total_ref, q_ref, out_ref, grad_ref, *refs, first_part, n_parts, n_blocks, groups, q_offset, fused
):
    key_refs, refs = refs[: 2 * n_parts], refs[2 * n_parts :]
    if fused:
        (all_ref, dk_acc, dv_acc) = refs
        columns = all_ref.shape[1] // 3
    else:
        (dq_ref, dkv_ref, dk_acc, dv_acc) = refs
        columns = dq_ref.shape[1]
    b = pl.program_id(0)

    @pl.when(b == 0)
    def _():
        dk_acc[...] = jnp.zeros_like(dk_acc)
        dv_acc[...] = jnp.zeros_like(dv_acc)

    q_rows, q_wide, g_rows, g_wide, inner, log_total = [], [], [], [], [], []
    for g in range(groups):
        queries = q_ref[:, pair(g)].astype(F32) * (HD**-0.5)
        q_rows.append(rows_of_two_heads(queries).astype(BF16))
        q_wide.append(columns_of_two_heads(queries).astype(BF16))
        grad = grad_ref[:, pair(g)].astype(F32)
        g_rows.append(rows_of_two_heads(grad).astype(BF16))
        g_wide.append(columns_of_two_heads(grad).astype(BF16))
        product = (grad * out_ref[:, pair(g)].astype(F32)).T
        inner.append(
            jnp.concatenate(
                [jnp.sum(product[:HD], axis=0, keepdims=True), jnp.sum(product[HD:], axis=0, keepdims=True)], axis=1
            )
        )
        log_total.append(total_ref[0, g : g + 1, :])
    dq = (jnp.zeros((2 * HD, 2 * BQ), F32),) * groups
    base = 0
    for part in range(n_parts):
        k_ref, v_ref = key_refs[2 * part], key_refs[2 * part + 1]
        first, last = mask_of(interval_ref, first_part + part, b)
        low, high = blocks_of(first, last, k_ref.shape[0])

        def step(j, dq, k_ref=k_ref, v_ref=v_ref, first=first, last=last, base=base):
            rows = pl.ds(pl.multiple_of(j * BK, BK), BK)
            sums = pl.ds(pl.multiple_of(base + j * BK, BK), BK)
            inside = seen(first, last, j)
            new = []
            for g in range(groups):
                keys = k_ref[rows, pair(g)]
                scores = jnp.dot(keys, q_wide[g], preferred_element_type=F32)
                prob_grad = jnp.dot(v_ref[rows, pair(g)], g_wide[g], preferred_element_type=F32)
                probs = jnp.exp(jnp.where(inside, scores, NEGATIVE) - log_total[g])
                score_grad = (probs * (prob_grad - inner[g])).astype(BF16)
                dv_acc[sums, pair(g)] += jnp.dot(probs.astype(BF16), g_rows[g], preferred_element_type=F32)
                dk_acc[sums, pair(g)] += jnp.dot(score_grad, q_rows[g], preferred_element_type=F32)
                new.append(
                    dq[g]
                    + lax.dot_general(keys, score_grad, (((0,), (0,)), ((), ())), preferred_element_type=F32)
                )
            return tuple(new)

        dq = lax.fori_loop(low, high, step, dq)
        base += k_ref.shape[0]
    for g in range(groups):
        value = (heads_side_by_side(dq[g]) * (HD**-0.5)).astype(BF16)
        if fused:
            all_ref[pl.ds(pl.multiple_of(q_offset + b * BQ, BQ), BQ), pair(g)] = value
        else:
            dq_ref[:, pair(g)] = value

    @pl.when(b == n_blocks - 1)
    def _():
        if fused:
            if q_offset:
                all_ref[:q_offset, :columns] = jnp.zeros((q_offset, columns), BF16)
            all_ref[:, columns : 2 * columns] = dk_acc[...].astype(BF16)
            all_ref[:, 2 * columns :] = dv_acc[...].astype(BF16)
        else:
            dkv_ref[:, :columns] = dk_acc[...].astype(BF16)
            dkv_ref[:, columns:] = dv_acc[...].astype(BF16)


def row_block(columns, index=0, offset=0):
    return pl.BlockSpec((BQ, columns), lambda b, *_: (b + offset // BQ, index))


def whole(shape):
    return pl.BlockSpec(shape, lambda *_: (0,) * len(shape))


def params(mib):
    return pltpu.CompilerParams(dimension_semantics=("arbitrary",), vmem_limit_bytes=mib << 20)


def attend_forward(intervals, first_part, columns, q, parts, q_offset):
    q_array, q_index = q
    n_blocks = intervals.shape[1]
    length, groups = n_blocks * BQ, columns // (2 * HD)
    operands, specs = [intervals, q_array], [whole(intervals.shape), row_block(columns, q_index, q_offset)]
    for part in parts:
        operands += list(part)
        specs += [whole(x.shape) for x in part]
    return pl.pallas_call(
        functools.partial(forward_kernel, first_part=first_part, n_parts=len(parts), groups=groups),
        grid=(n_blocks,),
        in_specs=specs,
        out_specs=[row_block(columns), pl.BlockSpec((1, groups, 2 * BQ), lambda b: (b, 0, 0))],
        out_shape=[
            jax.ShapeDtypeStruct((length, columns), BF16),
            jax.ShapeDtypeStruct((n_blocks, groups, 2 * BQ), F32),
        ],
        compiler_params=params(14),
        cost_estimate=COST,
        name="attend_forward",
    )(*operands)


def attend_backward(intervals, first_part, columns, totals, q, out, out_grad, parts, q_offset, fused):
    q_array, q_index = q
    n_blocks = intervals.shape[1]
    length, groups = n_blocks * BQ, columns // (2 * HD)
    operands = [intervals, totals, q_array, out, out_grad]
    specs = [
        whole(intervals.shape),
        pl.BlockSpec((1, groups, 2 * BQ), lambda b: (b, 0, 0)),
        row_block(columns, q_index, q_offset),
        row_block(columns),
        row_block(columns),
    ]
    for part in parts:
        operands += list(part)
        specs += [whole(x.shape) for x in part]
    n_keys = sum(keys.shape[0] for keys, _ in parts)
    if fused:
        out_specs = [whole((n_keys, 3 * columns))]
        out_shape = [jax.ShapeDtypeStruct((n_keys, 3 * columns), BF16)]
    else:
        out_specs = [row_block(columns), whole((n_keys, 2 * columns))]
        out_shape = [
            jax.ShapeDtypeStruct((length, columns), BF16),
            jax.ShapeDtypeStruct((n_keys, 2 * columns), BF16),
        ]
    return pl.pallas_call(
        functools.partial(
            backward_kernel,
            first_part=first_part,
            n_parts=len(parts),
            n_blocks=n_blocks,
            groups=groups,
            q_offset=q_offset,
            fused=fused,
        ),
        grid=(n_blocks,),
        in_specs=specs,
        out_specs=out_specs,
        scratch_shapes=[pltpu.VMEM((n_keys, columns), F32), pltpu.VMEM((n_keys, columns), F32)],
        out_shape=out_shape,
        compiler_params=params(18 if fused else 26),
        cost_estimate=COST,
        name="attend_backward",
    )(*operands)


COST = pl.CostEstimate(flops=1 << 20, bytes_accessed=1 << 20, transcendentals=0)


def inverse_rms(rows):
    return lax.rsqrt(jnp.mean(rows * rows, axis=-1, keepdims=True) + EPSILON)


def normalize(rows, gain):
    return rows * inverse_rms(rows) * gain


def normalize_back(rows, gain, cotangent):
    inverse = inverse_rms(rows)
    unit = rows * inverse
    scaled = cotangent * gain
    grad = inverse * (scaled - unit * jnp.mean(scaled * unit, axis=-1, keepdims=True))
    return grad, jnp.sum(cotangent * unit, axis=0)


def gelu_parts(u):
    c = float((2.0 / jnp.pi) ** 0.5)
    t = jnp.tanh(c * (u + 0.044715 * u * u * u))
    half = 0.5 * (1.0 + t)
    slope = half + 0.5 * u * (1.0 - t * t) * (c * (1.0 + 3.0 * 0.044715 * u * u))
    return u * half, slope


def contract(a, b, i, j):
    return lax.dot_general(a, b, (((i,), (j,)), ((), ())), preferred_element_type=F32)


def nn(a, b):
    return contract(a, b, 1, 0)


def nt(a, b):
    return contract(a, b, 1, 1)


def tn(a, b):
    return contract(a, b, 0, 0)


def dot(a, b, i, j):
    return lax.dot_general(a, b, (((i,), (j,)), ((), ())), preferred_element_type=F32)


class Part:
    def __init__(self, array, columns=None, at=0, plane=None, row=0):
        self.array, self.at, self.plane, self.row = array, at, plane, row
        self.columns = array.shape[-1] if columns is None else columns

    def split(self, rows):
        at, row = self.at, self.row // rows
        return pl.BlockSpec((rows, self.columns), lambda i, *_: (row + i, at))

    def spec(self):
        if self.plane is None:
            at = self.at
            return pl.BlockSpec((self.array.shape[0], self.columns), lambda *_: (0, at))
        plane = self.plane
        return pl.BlockSpec((None,) + self.array.shape[1:], lambda *_: (plane, 0, 0))


def back_kernel(*refs, n, m, norm, stacked):
    grads, weights, refs = refs[:n], refs[n : 2 * n], refs[2 * n :]
    total = dot(grads[0][...], weights[0][...], 1, 1)
    for grad, weight in zip(grads[1:], weights[1:]):
        total = total + dot(grad[...], weight[...], 1, 1)
    if not norm:
        add, out_ref = refs[:-1], refs[-1]
        for ref in add:
            total = total + ref[...].astype(F32)
        out_ref[...] = total.astype(out_ref.dtype)
        return
    resid_ref, gain_ref, base_ref = refs[:3]
    out_weights, (grad_ref, full_ref, gain_out), outs = refs[3 : 3 + m], refs[3 + m : 6 + m], refs[6 + m :]
    rows = resid_ref[...]
    inverse = inverse_rms(rows)
    unit = rows * inverse
    scaled = total * gain_ref[...]
    grad = base_ref[...].astype(F32) + inverse * (scaled - unit * jnp.mean(scaled * unit, axis=-1, keepdims=True))
    grad_ref[...] = grad
    full = grad.astype(BF16)
    full_ref[...] = full

    @pl.when(pl.program_id(0) == 0)
    def _():
        gain_out[...] = jnp.zeros_like(gain_out)

    gain_out[...] += jnp.sum(total * unit, axis=0, keepdims=True)
    for weight, out in zip(out_weights, outs):
        out[...] = dot(full, weight[...], 1, 1).astype(BF16)


TILE = 256


def product_back(pairs, length, dtype, add=None):
    n, features = len(pairs), pairs[0][1].array.shape[-2]
    grads, weights = zip(*pairs)
    add = [] if add is None else [add]
    return pl.pallas_call(
        functools.partial(back_kernel, n=n, m=0, norm=False, stacked=0),
        grid=(length // TILE,),
        in_specs=[g.split(TILE) for g in grads] + [w.spec() for w in weights] + [Part(x).split(TILE) for x in add],
        out_specs=pl.BlockSpec((TILE, features), lambda i: (i, 0)),
        out_shape=jax.ShapeDtypeStruct((length, features), dtype),
        compiler_params=params(30),
        cost_estimate=COST,
        name="back",
    )(*[p.array for p in grads], *in_hbm([p.array for p in weights]), *add)


def norm_back(pairs, resid, gain, base, out_weights):
    n, m, (length, features) = len(pairs), len(out_weights), resid.shape
    grads, weights = zip(*pairs)
    tile = lambda x: Part(x).split(TILE)
    widths = [w.shape[0] for w in out_weights]
    return pl.pallas_call(
        functools.partial(back_kernel, n=n, m=m, norm=True, stacked=0),
        grid=(length // TILE,),
        in_specs=[g.split(TILE) for g in grads]
        + [w.spec() for w in weights]
        + [tile(resid), whole((1, features)), tile(base)]
        + [whole(w.shape) for w in out_weights],
        out_specs=[pl.BlockSpec((TILE, features), lambda i: (i, 0))] * 2
        + [whole((1, features))]
        + [pl.BlockSpec((TILE, w), lambda i: (i, 0)) for w in widths],
        out_shape=[
            jax.ShapeDtypeStruct((length, features), F32),
            jax.ShapeDtypeStruct((length, features), BF16),
            jax.ShapeDtypeStruct((1, features), F32),
        ]
        + [jax.ShapeDtypeStruct((length, w), BF16) for w in widths],
        compiler_params=params(34),
        cost_estimate=COST,
        name="norm_back",
    )(*[p.array for p in grads], *[p.array for p in weights], resid, gain.reshape(1, -1), base, *out_weights)


def weight_kernel(*refs, n, m):
    rows, grads, outs, turned = refs[:n], refs[n : n + m], refs[n + m : n + 2 * m], refs[-1]

    @pl.when(pl.program_id(0) == 0)
    def _():
        at = 0
        for ref in rows:
            for first in range(0, ref.shape[0], TILE):
                turned[:, at + first : at + first + TILE] = ref[first : first + TILE, :].astype(F32).T.astype(BF16)
            at += ref.shape[0]

    for grad, out in zip(grads, outs):
        out[...] = dot(turned[...], grad[...], 1, 0).astype(BF16)


def weight_grads(rows, grads, chunk):
    length, features = sum(x.shape[0] for x in rows), rows[0].shape[1]
    columns = grads[0].shape[1]
    return pl.pallas_call(
        functools.partial(weight_kernel, n=len(rows), m=len(grads)),
        grid=(columns // chunk,),
        in_specs=[whole(x.shape) for x in rows]
        + [pl.BlockSpec((length, chunk), lambda j: (0, j)) for _ in grads],
        out_specs=[pl.BlockSpec((features, chunk), lambda j: (0, j)) for _ in grads],
        out_shape=[jax.ShapeDtypeStruct((features, columns), BF16) for _ in grads],
        scratch_shapes=[pltpu.VMEM((features, length), BF16)],
        compiler_params=params(30),
        cost_estimate=COST,
        name="weight_grads",
    )(*rows, *grads)


def ffn_kernel(normed_ref, full_ref, gate_ref, up_ref, down_ref, hidden_ref, grads_ref, *, chunk, units):
    j = pl.program_id(0)
    gate = dot(normed_ref[...], gate_ref[...], 1, 0)
    up = dot(normed_ref[...], up_ref[...], 1, 0)
    hidden_grad = dot(full_ref[...], down_ref[...], 1, 1)
    act, slope = gelu_parts(gate)
    hidden_ref[...] = (act * up).astype(BF16)
    at = pl.multiple_of(j * chunk, chunk)
    grads_ref[:, pl.ds(at, chunk)] = (hidden_grad * up * slope).astype(BF16)
    grads_ref[:, pl.ds(pl.multiple_of(units + at, chunk), chunk)] = (hidden_grad * act).astype(BF16)


def feed_forward(normed, full, gate, up, down, chunk=256):
    (length, features), units = normed.shape, down.shape[0]

    def columns(part):
        if part.plane is None:
            first = part.at * part.columns // chunk
            return pl.BlockSpec((features, chunk), lambda j: (0, first + j))
        plane = part.plane
        return pl.BlockSpec((None, features, chunk), lambda j: (plane, 0, j))

    return pl.pallas_call(
        functools.partial(ffn_kernel, chunk=chunk, units=units),
        grid=(units // chunk,),
        in_specs=[
            whole(normed.shape),
            whole(full.shape),
            columns(gate),
            columns(up),
            pl.BlockSpec((chunk, features), lambda j: (j, 0)),
        ],
        out_specs=[pl.BlockSpec((length, chunk), lambda j: (0, j)), whole((length, 2 * units))],
        out_shape=[
            jax.ShapeDtypeStruct((length, units), BF16),
            jax.ShapeDtypeStruct((length, 2 * units), BF16),
        ],
        compiler_params=params(24),
        cost_estimate=COST,
        name="feed_forward",
    )(normed, full, *in_hbm([gate.array, up.array, down]))


def in_hbm(arrays):
    return [pltpu.with_memory_space_constraint(x, pltpu.HBM) for x in arrays]


def tie(x, *others):
    return lax.optimization_barrier((x, others))[0] if others else x


def arrange_kernel(scalars, mine_ref, theirs_ref, *out_refs, outputs):
    top = scalars[1]
    at = 0
    for out_ref, (width, planes) in zip(out_refs, outputs):
        for plane in range(max(planes, 1)):
            mine, theirs = (ref[0, :, at : at + width].astype(out_ref.dtype) for ref in (mine_ref, theirs_ref))
            at += width
            if planes:
                out_ref[plane, top, 0] = mine
                out_ref[plane, 1 - top, 0] = theirs
            else:
                out_ref[0, :, :width] = jnp.where(top == 0, mine, theirs)
                out_ref[0, :, width:] = jnp.where(top == 0, theirs, mine)


def arrange(mine, theirs, index, top, outputs, dtype):
    n, rows, columns = mine.shape
    scalars = jnp.stack([index, top]).astype(jnp.int32)
    specs, shapes = [], []
    for w, planes in outputs:
        if planes:
            specs.append(pl.BlockSpec((planes, 2, 1, rows, w), lambda i, sc: (0, 0, i, 0, 0)))
            shapes.append(jax.ShapeDtypeStruct((planes, 2, n, rows, w), dtype))
        else:
            specs.append(pl.BlockSpec((1, rows, 2 * w), lambda i, sc: (i, 0, 0)))
            shapes.append(jax.ShapeDtypeStruct((n, rows, 2 * w), dtype))
    outs = pl.pallas_call(
        functools.partial(arrange_kernel, outputs=outputs),
        grid_spec=pltpu.PrefetchScalarGridSpec(
            num_scalar_prefetch=1,
            grid=(n,),
            in_specs=[pl.BlockSpec((1, rows, columns), lambda i, sc: (i ^ sc[0], 0, 0))] * 2,
            out_specs=specs,
        ),
        out_shape=shapes,
        compiler_params=params(12),
        cost_estimate=COST,
        name="arrange",
    )(scalars, mine, theirs)
    return [
        x.reshape(x.shape[0], 2 * n * rows, w) if planes else x.reshape(n * rows, 2 * w)
        for x, (w, planes) in zip(outs, outputs)
    ]


class Links:
    def __init__(self, n_dp):
        self.n_dp = n_dp
        self.n_bits = n_dp.bit_length() - 1
        self.here = lax.axis_index("dp")

    def bit(self, k):
        return (self.here >> k) & 1

    def across_tp(self, x):
        return lax.ppermute(x, "tp", [(0, 1), (1, 0)])

    def across(self, x, mask):
        return lax.ppermute(x, "dp", [(i, i ^ mask) for i in range(self.n_dp)])


class Single:
    def __init__(self, move):
        self.move, self.started = move, False

    def send(self, x, *after):
        self.sent = tie(x, *after)
        self.got = [self.move(self.sent)]

    def take(self):
        return self.got[0]


class Fetch:
    def __init__(self, links, shards, bits, outputs):
        self.links, self.bits, self.outputs = links, list(bits), outputs
        self.n, self.index, self.got, self.held = 1 << len(bits), 0, None, None
        for place, k in enumerate(bits):
            self.index = self.index + (links.bit(k) << place)
        self.piece = jnp.concatenate([y for x in shards for y in self.pieces(x)], axis=2)

    def pieces(self, x):
        if isinstance(x, tuple):
            (x,) = x
            rows, columns, half = x.shape[0] * 2 // self.n, x.shape[1] // 2, self.n // 2
            at = (self.index % half * rows, self.index // half * columns)
            return [lax.dynamic_slice(x, at, (rows, columns))[None]]
        x = x.reshape(-1, self.n, x.shape[-2] // self.n, x.shape[-1])
        return list(lax.dynamic_slice_in_dim(x, self.index, 1, axis=1))

    def send(self, *after):
        if self.held is None:
            self.sent = tie(self.piece, *after)
            self.got = [self.links.across_tp(self.sent)]
        else:
            self.sent = tie(self.held, *after)
            self.got = [self.links.across(self.sent, 1 << self.bits[0])]

    def take(self):
        if self.held is None:
            self.held = self.got[0]
            return
        self.bits.pop(0)
        if self.bits:
            self.held = jnp.concatenate([self.held, self.got[0]], axis=0)
            if len(self.bits) == 1:
                self.last = self.bits[0]
        else:
            self.theirs = self.got[0]

    def ended(self):
        return not self.bits

    def finish(self):
        top, below = self.links.bit(self.last), self.index & (self.n // 2 - 1)
        whole_arrays = arrange(self.held, self.theirs, below, top, self.outputs, BF16)
        return [x[0] if x.ndim == 3 and x.shape[0] == 1 else x for x in whole_arrays]


TP = "tp"
HALO, PROJECT, MEMORY, GATE, DOWN, REST, CROSS, SELF = range(8)


class Reduction:
    def __init__(self, links, own, other, order, outputs):
        self.links, self.order, self.outputs = links, list(order), outputs
        self.back = [k for k in reversed(order) if k is not TP][:-1]
        self.n_blocks = links.n_dp
        view = lambda x: x.reshape(self.n_blocks, -1, x.shape[-1])
        self.own, self.other = [([view(x) for x in own], 0)], [([view(x) for x in other], 0)]
        self.at, self.size = 0, self.n_blocks
        self.index = 0
        self.result = self.theirs = None

    def piece(self, addends, at, size):
        total = 0.0
        for arrays, base in addends:
            parts = [lax.dynamic_slice_in_dim(x, at - base, size).astype(F32) for x in arrays]
            total = total + (jnp.concatenate(parts, axis=2) if len(parts) > 1 else parts[0])
        return total.astype(BF16)

    def send(self, *after):
        links = self.links
        if self.result is not None:
            bits = self.back[0] if self.back else (0,)
            masks = self.masks(bits)
            self.sent = tie(self.result, *after)
            self.got = [links.across(self.sent, mask) for mask in masks]
        elif self.order[0] is TP:
            self.sent = tie(self.piece(self.other, self.at, self.size), *after)
            self.got = [links.across_tp(self.sent)]
            self.other = None
        else:
            bits = self.order[0]
            masks = self.masks(bits)
            digit = 0
            for k in bits:
                digit = digit * 2 + links.bit(k)
            part = self.size // (len(masks) + 1)
            self.got, self.sent = [], []
            for i, mask in enumerate(masks):
                at = self.at + (digit ^ (i + 1)) * part
                sent = self.piece(self.own, at, part)
                if self.other is not None:
                    sent = jnp.concatenate([sent, self.piece(self.other, at, part)], axis=0)
                self.sent.append(tie(sent, *after))
                self.got.append(links.across(self.sent[-1], mask))
            self.at, self.size = self.at + digit * part, part
            if bits != (0,):
                self.index = self.index * (len(masks) + 1) + digit
        return self.got

    def masks(self, bits):
        out = []
        for i in range(1, 1 << len(bits)):
            out.append(sum(1 << k for place, k in enumerate(reversed(bits)) if (i >> place) & 1))
        return out

    def take(self):
        if self.result is not None:
            if self.back:
                self.back.pop(0)
                self.result = jnp.concatenate([self.result] + self.got, axis=0)
            else:
                self.theirs = self.got[0]
            return self.result
        self.order.pop(0)
        for got in self.got:
            self.own = self.own + [([got[: self.size]], self.at)]
            if self.other is not None:
                self.other = self.other + [([got[self.size :]], self.at)]
        if not self.order:
            self.result = self.piece(self.own, self.at, self.size)
        return self.got

    def ended(self):
        return self.theirs is not None

    def finish(self):
        return arrange(self.result, self.theirs, self.index, self.links.bit(0), self.outputs, F32)


class Agenda:
    def __init__(self, links):
        self.links, self.chains, self.now, self.strict = links, {}, (), True

    def at(self, x):
        return tie(x, *self.now)

    def after(self, *values):
        self.now = values

    def start(self, name, chain, *args):
        self.chains[name] = chain
        chain.send(*args, *self.now)
        self.now = (self.now, chain.sent)

    def go(self, name):
        chain = self.chains[name]
        if self.strict:
            chain.got = tie(chain.got, *self.now)
        came = chain.got
        chain.take()
        if chain.ended():
            self.now = (came,)
            return chain.finish()
        chain.send(came, *self.now)
        self.now = (came, chain.sent)

    def take(self, name):
        came = self.chains[name].take()
        if self.strict:
            came = tie(came, *self.now)
        self.now = (self.now, came)
        return came


def column_halves(x):
    half = x.shape[1] // 2
    return jnp.concatenate([x[:, :half], x[:, half:]], axis=0)


def beside(x):
    return jnp.concatenate(list(x), axis=1)


def shards(
    n_dp,
    decoder_rows,
    memory_rows,
    output_grad,
    token_segments,
    memory_segments,
    valid_mask,
    norm_gains,
    self_project,
    self_output,
    cross_query,
    cross_memory,
    cross_output,
    gate_up,
    down_weight,
):
    links = Links(n_dp)
    side = lax.axis_index("tp")
    decoder, memory, out_grad = decoder_rows[0], memory_rows[0], output_grad[0]
    valid = valid_mask[0]
    own_len, features = decoder.shape
    mem_len, columns = memory.shape[0], cross_query.shape[1]
    halo = token_segments.shape[1] // 4
    both = (0, 1)

    d, units = features, down_weight.shape[0]
    half_len = mem_len // 2
    agenda = Agenda(links)
    at, after, start, go, take = agenda.at, agenda.after, agenda.start, agenda.go, agenda.take
    v = types.SimpleNamespace()
    v.kv_own_of = [None, None]
    v.self_of = [None, None]
    v.cross_of = [None, None]
    v.query_grad_of = [None, None]
    v.kv_grad_of = [None, None]
    v.memory_dw_of = [None, None]
    v.proj_grad_of = [None, None]
    v.memory_came, v.memory_got = [], []
    bit0, bit1, rest = (0,), (1,), [(k,) for k in range(2, links.n_bits)]
    tp_first, tp_second, tp_third = (
        [bit0, TP, bit1] + rest,
        [bit0, bit1, TP] + rest,
        [bit0, bit1] + rest[:1] + [TP] + rest[1:],
    )
    resid0 = decoder.astype(F32)
    valid_rows = valid.astype(F32)[:, None]
    grad_m = out_grad.astype(F32) * valid_rows
    full_m = grad_m.astype(BF16)

    def sums(name, order, outputs, parts):
        after(parts)
        start(name, Reduction(links, *parts, order, outputs))

    def send_halo():
        start(HALO, Single(lambda x: lax.ppermute(x, "tp", [(0, 1)])), decoder[-halo:])

    def send_project():
        start(PROJECT, Fetch(links, [self_project], BITS, ((columns, 3),)))

    def send_memory(i):
        start(MEMORY, Single(links.across_tp), memory)

    def send_ffn():
        def mine(x):
            blocks = x.reshape(-1, links.n_dp, x.shape[-2] // links.n_dp, x.shape[-1])
            return jnp.concatenate(list(lax.dynamic_index_in_dim(blocks, links.here, 1, False)), axis=1)

        start(GATE, Single(links.across_tp), mine(gate_up))
        start(DOWN, Single(links.across_tp), mine(down_weight))

    def gather_ffn():
        gate_other = lax.all_gather(take(GATE), "dp", axis=0, tiled=True)
        v.gate_w = [Part(gate_up, plane=c) for c in both], [Part(gate_other, units, c) for c in both]
        v.down_w = (down_weight, lax.all_gather(take(DOWN), "dp", axis=0, tiled=True))

    def send_rest():
        start(
            REST,
            Fetch(
                links,
                [cross_memory, cross_query, (self_output,), (cross_output,)],
                BITS,
                ((columns, 2), (columns, 1), (columns, 0), (columns, 0)),
            ),
        )

    def plan():
        v.intervals = make_plans(side, token_segments, memory_segments, own_len, mem_len, halo)
        after(v.intervals)

    def norm_a():
        v.rows_a = jnp.concatenate([take(HALO), decoder], axis=0).astype(F32)
        v.normed_a = normalize(v.rows_a, norm_gains[0]).astype(BF16)

    def self_forward(h):
        if h:
            v.project = (self_project, out[PROJECT][0])
        weights = v.project[1] if h else self_project
        rows = at(v.normed_a)
        proj = [nn(rows, weights[c]).astype(BF16) for c in range(3)]
        att, totals = attend_forward(v.intervals, 0, columns, (proj[0], 0), ((proj[1], proj[2]),), halo)
        v.self_of[h] = proj, att, totals
        after(att)

    def keys_of(rows, h):
        return tuple(nn(rows, v.memory_w[h][c]).astype(BF16) for c in both)

    def keys_own(h):
        v.kv_own_of[h] = keys_of(at(memory), h)
        after(v.kv_own_of[h])

    def weights_rest():
        other_memory, other_query, other_out_a, other_out_c = out[REST]
        v.memory_w = (cross_memory, other_memory)
        v.out_a, v.out_c, v.query_w = (
            (self_output, other_out_a),
            (cross_output, other_out_c),
            (cross_query, other_query),
        )

    def queries():
        weights_rest()
        v.proj_a, v.att_a, v.totals_a = zip(*v.self_of)
        att = at(v.att_a)
        v.branch_a = nn(att[0], v.out_a[0]) + nn(att[1], v.out_a[1])
        v.resid1 = resid0 + v.branch_a
        v.normed_c = normalize(v.resid1, norm_gains[1]).astype(BF16)
        v.query_c = [nn(v.normed_c, v.query_w[h]).astype(BF16) for h in both]
        after(v.query_c)

    def take_memory():
        v.memory_came.append(take(MEMORY))

    def cross_forward(h):
        if not h:
            (v.memory_other,) = v.memory_came
        keys = (v.kv_own_of[h], keys_of(at(v.memory_other), h))
        att, totals = attend_forward(v.intervals, 1, columns, (v.query_c[h], 0), keys, 0)
        v.cross_of[h] = keys, att, totals
        after(att)

    def ffn():
        v.keys_c, v.att_c, v.totals_c = zip(*v.cross_of)
        att = at(v.att_c)
        v.branch_c = nn(att[0], v.out_c[0]) + nn(att[1], v.out_c[1])
        v.resid2 = v.resid1 + v.branch_c
        v.normed_m = normalize(v.resid2, norm_gains[2]).astype(BF16)
        v.hidden, v.gate_grads = zip(
            *[feed_forward(v.normed_m, full_m, *v.gate_w[h], v.down_w[h]) for h in both]
        )
        after(v.gate_grads)

    def gate_dw():
        agenda.strict = False
        parts = weight_grads([v.normed_m], at(list(v.gate_grads)), 512)
        sums(GATE, ORDERS[GATE], ((units, 2),), [[x] for x in parts])

    def down_dw():
        v.down_dw = weight_grads([at(full_m)], list(v.hidden), 512)
        after(v.down_dw)

    def norm_m_grad():
        v.gate_late = at(v.gate_grads)

    def norm_m_back():
        pairs = [(Part(v.gate_late[h], units, c), v.gate_w[h][c]) for h in both for c in both]
        v.grad_c, v.full_c, gain, *v.att_c_grad = norm_back(pairs, v.resid2, norm_gains[2], full_m, v.out_c)
        v.gain_m = gain[0]
        after(v.att_c_grad)

    def outs_dw():
        grad = at(v.full_c)
        out_dw = [weight_grads([v.att_c[h]], [grad], grad.shape[1])[0] for h in both]
        parts = [[v.down_dw[h], column_halves(out_dw[h])] for h in both]
        sums(DOWN, ORDERS[DOWN], ((units, 1), (columns, 0)), parts)

    def cross_backward(h):
        grad = at(v.att_c_grad[h])
        query = (v.query_c[h], 0)
        v.query_grad_of[h], v.kv_grad_of[h] = attend_backward(
            v.intervals, 1, columns, v.totals_c[h], query, v.att_c[h], grad, v.keys_c[h], 0, False
        )
        after(v.query_grad_of[h])

    def norm_c_back():
        grads = at(v.query_grad_of)
        pairs = [(Part(grads[h]), Part(v.query_w[h])) for h in both]
        v.grad_a, v.full_a, gain, *v.att_a_grad = norm_back(pairs, v.resid1, norm_gains[1], v.grad_c, v.out_a)
        v.gain_c = gain[0]
        after(v.att_a_grad)

    def memory_back(own):
        kv = at(v.kv_grad_of)
        row = 0 if own else mem_len
        pairs = [(Part(kv[h], columns, c, row=row), Part(v.memory_w[h], plane=c)) for h in both for c in both]
        if own:
            v.memory_grad = product_back(pairs, mem_len, F32, v.memory_got[0])
            after(v.memory_grad)
        else:
            v.memory_partial = product_back(pairs, mem_len, BF16)
            after(v.memory_partial)

    def send_partial(i):
        start(MEMORY, Single(links.across_tp), v.memory_partial)

    def take_partial():
        v.memory_got.append(take(MEMORY))

    def memory_dw(h):
        if h:
            v.memory_dw_of = weight_grads([memory, v.memory_other], at(v.kv_grad_of), 384)
            after(v.memory_dw_of)

    def cross_dw():
        query_dw = weight_grads([at(v.normed_c)], v.query_grad_of, columns)
        out_dw = [weight_grads([v.att_a[h]], [at(v.full_a)], v.full_a.shape[1])[0] for h in both]
        parts = [[v.memory_dw_of[h], query_dw[h], column_halves(out_dw[h])] for h in both]
        sums(CROSS, ORDERS[CROSS], ((columns, 2), (columns, 1), (columns, 0)), parts)

    def self_backward(h):
        grad = at(v.att_a_grad[h])
        proj, *keys = v.proj_a[h]
        v.proj_grad_of[h] = attend_backward(
            v.intervals, 0, columns, v.totals_a[h], (proj, 0), v.att_a[h], grad, (keys,), halo, True
        )[0]
        after(v.proj_grad_of[h])

    def norm_a_grad():
        grads = at(v.proj_grad_of)
        pairs = [(Part(grads[h], columns, c), Part(v.project[h], plane=c)) for h in both for c in range(3)]
        v.normed_a_grad = total = product_back(pairs, own_len + halo, F32)
        after(total)
        start(HALO, Single(lambda x: lax.ppermute(x, "tp", [(1, 0)])), total[:halo].astype(BF16))
        v.branch_m = nn(v.hidden[0], v.down_w[0]) + nn(v.hidden[1], v.down_w[1])
        v.result = v.resid2 + v.branch_m
        gain_a = jnp.sum(total * v.rows_a * inverse_rms(v.rows_a), axis=0)
        rows = [jnp.sum(x * x * valid_rows, axis=0) for x in (v.result, v.branch_a, v.branch_c, v.branch_m)]
        rows += [jnp.sum(jnp.broadcast_to(valid_rows, resid0.shape), axis=0), v.gain_m, v.gain_c, gain_a]
        v.stats = jnp.pad(jnp.stack(rows), ((0, 2 * HD - len(rows)), (0, 0))).T.astype(BF16)

    def self_dw():
        parts = [[x, v.stats] for x in weight_grads([v.normed_a], at(v.proj_grad_of), 384)]
        sums(SELF, ORDERS[SELF], ((columns, 3), (2 * HD, 1)), parts)

    def norm_a_back():
        came = take(HALO).astype(F32)
        own = at(v.normed_a_grad[halo:])
        own = jnp.concatenate([own[:-halo], own[-halo:] + came], axis=0)
        resid0_grad, _ = normalize_back(resid0, norm_gains[0], own)
        v.decoder_grad = v.grad_a + resid0_grad
        after(v.decoder_grad)

    BITS = (1, 0)
    ORDERS = {GATE: tp_first, DOWN: tp_second, CROSS: tp_second, SELF: tp_first}
    v.memory_w = (None, None)
    out = {}

    def keys_first():
        v.memory_w = (cross_memory, None)
        keys_own(0)

    def advance(name):
        came = go(name)
        if came is not None:
            if name == DOWN:
                came[0] = came[0][0].T
            out[name] = came
            after(came)

    def for_each(block):
        return [functools.partial(block, h) for h in both]

    mem0, mem1 = for_each(send_memory)
    self0, self1 = for_each(self_forward)
    keys0, keys1 = keys_first, functools.partial(keys_own, 1)
    cross0, cross1 = for_each(cross_forward)
    cross_b0, cross_b1 = for_each(cross_backward)
    part0, part1 = for_each(send_partial)
    mem_dw0, mem_dw1 = for_each(memory_dw)
    self_b0, self_b1 = for_each(self_backward)
    mem_b0, mem_b1 = for_each(memory_back)
    P_, R, A, B, E, D = [functools.partial(advance, name) for name in (PROJECT, REST, GATE, DOWN, CROSS, SELF)]
    agenda_steps = (
        send_halo, send_project, send_ffn, plan, norm_a, P_, gather_ffn, send_rest, self0, P_, mem0, R, keys0, P_,
        self1, R, R, take_memory, queries, keys1, cross0, cross1, ffn, gate_dw, down_dw, norm_m_grad, A, norm_m_back,
        outs_dw, cross_b0, B, cross_b1, A, norm_c_back, mem_b0, part0, B, mem_dw0, mem_dw1, cross_dw, A, B, self_b1,
        E, A, B, self_b0, A, B, norm_a_grad, self_dw, E, A, B, take_partial, D, mem_b1, A, B, norm_a_back, E, D, A, B,
        E, D, A, E, D, B, E, D, E, D, E, D, E, D, D,
    )
    for step in agenda_steps:
        step()
    for name in (GATE, DOWN, CROSS, SELF):
        while name not in out:
            advance(name)

    stats = out[SELF][1][0, :, :8].T
    gains_grad = jnp.stack([stats[7], stats[6], stats[5]])
    root_squares = jnp.sqrt(jnp.sum(stats[:4], axis=1) / jnp.sum(stats[4]))
    return (
        v.result.astype(BF16)[None],
        v.decoder_grad[None],
        v.memory_grad[None],
        root_squares,
        gains_grad,
        out[SELF][0],
        out[CROSS][2],
        out[CROSS][1][0],
        out[CROSS][0],
        out[DOWN][1],
        out[GATE][0],
        out[DOWN][0],
    )


def solution(mesh):
    assert mesh.shape["tp"] == 2
    return jax.shard_map(
        functools.partial(shards, mesh.shape["dp"]),
        mesh=mesh,
        in_specs=(
            P("dp", "tp", None),
            P("dp", "tp", None),
            P("dp", "tp", None),
            P("dp", None),
            P("dp", None),
            P("dp", "tp"),
            P(),
            P(None, None, "tp"),
            P("tp", None),
            P(None, "tp"),
            P(None, None, "tp"),
            P("tp", None),
            P(None, None, "tp"),
            P("tp", None),
        ),
        out_specs=(
            P("dp", "tp", None),
            P("dp", "tp", None),
            P("dp", "tp", None),
            P(),
            P(),
            P(None, None, "tp"),
            P("tp", None),
            P(None, "tp"),
            P(None, None, "tp"),
            P("tp", None),
            P(None, None, "tp"),
            P("tp", None),
        ),
        check_vma=False,
    )
```

```python
import functools
import types

import jax
import jax.numpy as jnp
from jax import lax
from jax.experimental import pallas as pl
from jax.experimental.pallas import tpu as pltpu
from jax.sharding import PartitionSpec as P

HD = 64
EPSILON = 1e-06
NEGATIVE = -1e30
BQ = 128
BK = 256
F32 = jnp.float32
BF16 = jnp.bfloat16


def rows_of_two_heads(block):
    lane = lax.broadcasted_iota(jnp.int32, block.shape, 1)
    zero = jnp.zeros_like(block)
    return jnp.concatenate([jnp.where(lane < HD, block, zero), jnp.where(lane >= HD, block, zero)], axis=0)


def heads_side_by_side(wide):
    return jnp.concatenate([wide[:HD, :BQ], wide[HD:, BQ:]], axis=0).T


def columns_of_two_heads(block):
    turned = block.T
    row = lax.broadcasted_iota(jnp.int32, turned.shape, 0)
    zero = jnp.zeros_like(turned)
    return jnp.concatenate([jnp.where(row < HD, turned, zero), jnp.where(row >= HD, turned, zero)], axis=1)


def twice(row):
    return jnp.concatenate([row, row], axis=1)


def pair(g):
    return slice(2 * HD * g, 2 * HD * (g + 1))


def mask_of(interval_ref, part, b):
    first = interval_ref[2 * part, pl.ds(b, 1), :]
    last = interval_ref[2 * part + 1, pl.ds(b, 1), :]
    return twice(first), twice(last)


def blocks_of(first, last, n_keys):
    low = jnp.min(first.astype(F32)).astype(jnp.int32)
    high = jnp.max(last.astype(F32)).astype(jnp.int32)
    return jnp.clip(low, 0, n_keys) // BK, (jnp.clip(high, 0, n_keys) + BK - 1) // BK


def seen(first, last, j):
    key_iota = lax.broadcasted_iota(jnp.int32, (BK, 2 * BQ), 0)
    return (key_iota >= first - j * BK) & (key_iota < last - j * BK)


def plan_kernel(side_ref, tokens_ref, patches_ref, interval_ref, *, own_len, mem_len, halo):
    side = side_ref[0]
    first_own = side * own_len - halo
    n_blocks = own_len // BQ
    tokens, patches = tokens_ref[...], patches_ref[...]
    tokens_below, patches_below = [], []
    for segment in range(9):
        tokens_below.append(jnp.sum((tokens < segment).astype(F32), axis=1, keepdims=True))
        patches_below.append(jnp.sum((patches < segment).astype(F32), axis=1, keepdims=True))
    for b in range(n_blocks):
        own = tokens_ref[:, pl.ds(pl.multiple_of(side * own_len + b * BQ, BQ), BQ)]
        start_a, start_c, end_c = (jnp.zeros((1, BQ), F32) for _ in range(3))
        for segment in range(8):
            here = own == segment
            start_a = jnp.where(here, tokens_below[segment], start_a)
            start_c = jnp.where(here, patches_below[segment], start_c)
            end_c = jnp.where(here, patches_below[segment + 1], end_c)
        start_a, start_c, end_c = (x.astype(jnp.int32) for x in (start_a, start_c, end_c))
        place = lax.broadcasted_iota(jnp.int32, (1, BQ), 1) + (b * BQ + halo + 1)
        own_base, other_base = side * mem_len, (1 - side) * mem_len
        rows = (
            start_a - first_own,
            place,
            start_c - own_base,
            end_c - own_base,
            start_c - other_base,
            end_c - other_base,
        )
        for i, row in enumerate(rows):
            interval_ref[i, b : b + 1, :] = row


def make_plans(side, tokens, patches, own_len, mem_len, halo):
    intervals = pl.pallas_call(
        functools.partial(plan_kernel, own_len=own_len, mem_len=mem_len, halo=halo),
        grid_spec=pltpu.PrefetchScalarGridSpec(
            num_scalar_prefetch=1,
            grid=(1,),
            in_specs=[whole(tokens.shape), whole(patches.shape)],
            out_specs=whole((6, own_len // BQ, BQ)),
        ),
        out_shape=jax.ShapeDtypeStruct((6, own_len // BQ, BQ), jnp.int32),
        name="key_intervals",
    )(side.reshape(1).astype(jnp.int32), tokens, patches)
    return intervals


def forward_kernel(interval_ref, q_ref, *refs, first_part, n_parts, groups):
    key_refs, (out_ref, total_ref) = refs[: 2 * n_parts], refs[2 * n_parts :]
    b = pl.program_id(0)
    q_wide = []
    for g in range(groups):
        queries = q_ref[:, pair(g)].astype(F32) * (HD**-0.5)
        q_wide.append(columns_of_two_heads(queries).astype(BF16))
    carry = (
        (jnp.full((1, 2 * BQ), NEGATIVE, F32),) * groups,
        (jnp.zeros((1, 2 * BQ), F32),) * groups,
        (jnp.zeros((2 * HD, 2 * BQ), F32),) * groups,
    )
    for part in range(n_parts):
        k_ref, v_ref = key_refs[2 * part], key_refs[2 * part + 1]
        first, last = mask_of(interval_ref, first_part + part, b)
        low, high = blocks_of(first, last, k_ref.shape[0])

        def step(j, carry, k_ref=k_ref, v_ref=v_ref, first=first, last=last):
            rows = pl.ds(pl.multiple_of(j * BK, BK), BK)
            inside = seen(first, last, j)
            peaks, totals, accs = [], [], []
            scores = [
                jnp.where(inside, jnp.dot(k_ref[rows, pair(g)], q_wide[g], preferred_element_type=F32), NEGATIVE)
                for g in range(groups)
            ]
            for g in range(groups):
                peak, total, acc = (c[g] for c in carry)
                new_peak = jnp.maximum(peak, jnp.max(scores[g], axis=0, keepdims=True))
                shrink = jnp.exp(peak - new_peak)
                probs = jnp.exp(scores[g] - new_peak)
                peaks.append(new_peak)
                totals.append(total * shrink + jnp.sum(probs, axis=0, keepdims=True))
                accs.append(
                    acc * shrink
                    + lax.dot_general(
                        v_ref[rows, pair(g)],
                        probs.astype(BF16),
                        (((0,), (0,)), ((), ())),
                        preferred_element_type=F32,
                    )
                )
            return tuple(peaks), tuple(totals), tuple(accs)

        carry = lax.fori_loop(low, high, step, carry)
    for g in range(groups):
        peak, total, acc = (c[g] for c in carry)
        out_ref[:, pair(g)] = heads_side_by_side(acc / total).astype(BF16)
        total_ref[0, g : g + 1, :] = peak + jnp.log(total)


def backward_kernel(
    interval_ref, total_ref, q_ref, out_ref, grad_ref, *refs, first_part, n_parts, n_blocks, groups, q_offset, fused
):
    key_refs, refs = refs[: 2 * n_parts], refs[2 * n_parts :]
    if fused:
        (all_ref, dk_acc, dv_acc) = refs
        columns = all_ref.shape[1] // 3
    else:
        (dq_ref, dkv_ref, dk_acc, dv_acc) = refs
        columns = dq_ref.shape[1]
    b = pl.program_id(0)

    @pl.when(b == 0)
    def _():
        dk_acc[...] = jnp.zeros_like(dk_acc)
        dv_acc[...] = jnp.zeros_like(dv_acc)

    q_rows, q_wide, g_rows, g_wide, inner, log_total = [], [], [], [], [], []
    for g in range(groups):
        queries = q_ref[:, pair(g)].astype(F32) * (HD**-0.5)
        q_rows.append(rows_of_two_heads(queries).astype(BF16))
        q_wide.append(columns_of_two_heads(queries).astype(BF16))
        grad = grad_ref[:, pair(g)].astype(F32)
        g_rows.append(rows_of_two_heads(grad).astype(BF16))
        g_wide.append(columns_of_two_heads(grad).astype(BF16))
        product = (grad * out_ref[:, pair(g)].astype(F32)).T
        inner.append(
            jnp.concatenate(
                [jnp.sum(product[:HD], axis=0, keepdims=True), jnp.sum(product[HD:], axis=0, keepdims=True)], axis=1
            )
        )
        log_total.append(total_ref[0, g : g + 1, :])
    dq = (jnp.zeros((2 * HD, 2 * BQ), F32),) * groups
    base = 0
    for part in range(n_parts):
        k_ref, v_ref = key_refs[2 * part], key_refs[2 * part + 1]
        first, last = mask_of(interval_ref, first_part + part, b)
        low, high = blocks_of(first, last, k_ref.shape[0])

        def step(j, dq, k_ref=k_ref, v_ref=v_ref, first=first, last=last, base=base):
            rows = pl.ds(pl.multiple_of(j * BK, BK), BK)
            sums = pl.ds(pl.multiple_of(base + j * BK, BK), BK)
            inside = seen(first, last, j)
            new = []
            for g in range(groups):
                keys = k_ref[rows, pair(g)]
                scores = jnp.dot(keys, q_wide[g], preferred_element_type=F32)
                prob_grad = jnp.dot(v_ref[rows, pair(g)], g_wide[g], preferred_element_type=F32)
                probs = jnp.exp(jnp.where(inside, scores, NEGATIVE) - log_total[g])
                score_grad = (probs * (prob_grad - inner[g])).astype(BF16)
                dv_acc[sums, pair(g)] += jnp.dot(probs.astype(BF16), g_rows[g], preferred_element_type=F32)
                dk_acc[sums, pair(g)] += jnp.dot(score_grad, q_rows[g], preferred_element_type=F32)
                new.append(
                    dq[g]
                    + lax.dot_general(keys, score_grad, (((0,), (0,)), ((), ())), preferred_element_type=F32)
                )
            return tuple(new)

        dq = lax.fori_loop(low, high, step, dq)
        base += k_ref.shape[0]
    for g in range(groups):
        value = (heads_side_by_side(dq[g]) * (HD**-0.5)).astype(BF16)
        if fused:
            all_ref[pl.ds(pl.multiple_of(q_offset + b * BQ, BQ), BQ), pair(g)] = value
        else:
            dq_ref[:, pair(g)] = value

    @pl.when(b == n_blocks - 1)
    def _():
        if fused:
            if q_offset:
                all_ref[:q_offset, :columns] = jnp.zeros((q_offset, columns), BF16)
            all_ref[:, columns : 2 * columns] = dk_acc[...].astype(BF16)
            all_ref[:, 2 * columns :] = dv_acc[...].astype(BF16)
        else:
            dkv_ref[:, :columns] = dk_acc[...].astype(BF16)
            dkv_ref[:, columns:] = dv_acc[...].astype(BF16)


def row_block(columns, index=0, offset=0):
    return pl.BlockSpec((BQ, columns), lambda b, *_: (b + offset // BQ, index))


def whole(shape):
    return pl.BlockSpec(shape, lambda *_: (0,) * len(shape))


def params(mib):
    return pltpu.CompilerParams(dimension_semantics=("arbitrary",), vmem_limit_bytes=mib << 20)


def attend_forward(intervals, first_part, columns, q, parts, q_offset):
    q_array, q_index = q
    n_blocks = intervals.shape[1]
    length, groups = n_blocks * BQ, columns // (2 * HD)
    operands, specs = [intervals, q_array], [whole(intervals.shape), row_block(columns, q_index, q_offset)]
    for part in parts:
        operands += list(part)
        specs += [whole(x.shape) for x in part]
    return pl.pallas_call(
        functools.partial(forward_kernel, first_part=first_part, n_parts=len(parts), groups=groups),
        grid=(n_blocks,),
        in_specs=specs,
        out_specs=[row_block(columns), pl.BlockSpec((1, groups, 2 * BQ), lambda b: (b, 0, 0))],
        out_shape=[
            jax.ShapeDtypeStruct((length, columns), BF16),
            jax.ShapeDtypeStruct((n_blocks, groups, 2 * BQ), F32),
        ],
        compiler_params=params(14),
        cost_estimate=COST,
        name="attend_forward",
    )(*operands)


def attend_backward(intervals, first_part, columns, totals, q, out, out_grad, parts, q_offset, fused):
    q_array, q_index = q
    n_blocks = intervals.shape[1]
    length, groups = n_blocks * BQ, columns // (2 * HD)
    operands = [intervals, totals, q_array, out, out_grad]
    specs = [
        whole(intervals.shape),
        pl.BlockSpec((1, groups, 2 * BQ), lambda b: (b, 0, 0)),
        row_block(columns, q_index, q_offset),
        row_block(columns),
        row_block(columns),
    ]
    for part in parts:
        operands += list(part)
        specs += [whole(x.shape) for x in part]
    n_keys = sum(keys.shape[0] for keys, _ in parts)
    if fused:
        out_specs = [whole((n_keys, 3 * columns))]
        out_shape = [jax.ShapeDtypeStruct((n_keys, 3 * columns), BF16)]
    else:
        out_specs = [row_block(columns), whole((n_keys, 2 * columns))]
        out_shape = [
            jax.ShapeDtypeStruct((length, columns), BF16),
            jax.ShapeDtypeStruct((n_keys, 2 * columns), BF16),
        ]
    return pl.pallas_call(
        functools.partial(
            backward_kernel,
            first_part=first_part,
            n_parts=len(parts),
            n_blocks=n_blocks,
            groups=groups,
            q_offset=q_offset,
            fused=fused,
        ),
        grid=(n_blocks,),
        in_specs=specs,
        out_specs=out_specs,
        scratch_shapes=[pltpu.VMEM((n_keys, columns), F32), pltpu.VMEM((n_keys, columns), F32)],
        out_shape=out_shape,
        compiler_params=params(18 if fused else 26),
        cost_estimate=COST,
        name="attend_backward",
    )(*operands)


COST = pl.CostEstimate(flops=1 << 20, bytes_accessed=1 << 20, transcendentals=0)


def inverse_rms(rows):
    return lax.rsqrt(jnp.mean(rows * rows, axis=-1, keepdims=True) + EPSILON)


def normalize(rows, gain):
    return rows * inverse_rms(rows) * gain


def normalize_back(rows, gain, cotangent):
    inverse = inverse_rms(rows)
    unit = rows * inverse
    scaled = cotangent * gain
    grad = inverse * (scaled - unit * jnp.mean(scaled * unit, axis=-1, keepdims=True))
    return grad, jnp.sum(cotangent * unit, axis=0)


def gelu_parts(u):
    c = float((2.0 / jnp.pi) ** 0.5)
    t = jnp.tanh(c * (u + 0.044715 * u * u * u))
    half = 0.5 * (1.0 + t)
    slope = half + 0.5 * u * (1.0 - t * t) * (c * (1.0 + 3.0 * 0.044715 * u * u))
    return u * half, slope


def contract(a, b, i, j):
    return lax.dot_general(a, b, (((i,), (j,)), ((), ())), preferred_element_type=F32)


def nn(a, b):
    return contract(a, b, 1, 0)


def nt(a, b):
    return contract(a, b, 1, 1)


def tn(a, b):
    return contract(a, b, 0, 0)


def dot(a, b, i, j):
    return lax.dot_general(a, b, (((i,), (j,)), ((), ())), preferred_element_type=F32)


class Part:
    def __init__(self, array, columns=None, at=0, plane=None, row=0):
        self.array, self.at, self.plane, self.row = array, at, plane, row
        self.columns = array.shape[-1] if columns is None else columns

    def split(self, rows):
        at, row = self.at, self.row // rows
        return pl.BlockSpec((rows, self.columns), lambda i, *_: (row + i, at))

    def spec(self):
        if self.plane is None:
            at = self.at
            return pl.BlockSpec((self.array.shape[0], self.columns), lambda *_: (0, at))
        plane = self.plane
        return pl.BlockSpec((None,) + self.array.shape[1:], lambda *_: (plane, 0, 0))


def back_kernel(*refs, n, m, norm, stacked):
    grads, weights, refs = refs[:n], refs[n : 2 * n], refs[2 * n :]
    total = dot(grads[0][...], weights[0][...], 1, 1)
    for grad, weight in zip(grads[1:], weights[1:]):
        total = total + dot(grad[...], weight[...], 1, 1)
    if not norm:
        add, out_ref = refs[:-1], refs[-1]
        for ref in add:
            total = total + ref[...].astype(F32)
        out_ref[...] = total.astype(out_ref.dtype)
        return
    resid_ref, gain_ref, base_ref = refs[:3]
    out_weights, (grad_ref, full_ref, gain_out), outs = refs[3 : 3 + m], refs[3 + m : 6 + m], refs[6 + m :]
    rows = resid_ref[...]
    inverse = inverse_rms(rows)
    unit = rows * inverse
    scaled = total * gain_ref[...]
    grad = base_ref[...].astype(F32) + inverse * (scaled - unit * jnp.mean(scaled * unit, axis=-1, keepdims=True))
    grad_ref[...] = grad
    full = grad.astype(BF16)
    full_ref[...] = full

    @pl.when(pl.program_id(0) == 0)
    def _():
        gain_out[...] = jnp.zeros_like(gain_out)

    gain_out[...] += jnp.sum(total * unit, axis=0, keepdims=True)
    for weight, out in zip(out_weights, outs):
        out[...] = dot(full, weight[...], 1, 1).astype(BF16)


TILE = 256


def product_back(pairs, length, dtype, add=None):
    n, features = len(pairs), pairs[0][1].array.shape[-2]
    grads, weights = zip(*pairs)
    add = [] if add is None else [add]
    return pl.pallas_call(
        functools.partial(back_kernel, n=n, m=0, norm=False, stacked=0),
        grid=(length // TILE,),
        in_specs=[g.split(TILE) for g in grads] + [w.spec() for w in weights] + [Part(x).split(TILE) for x in add],
        out_specs=pl.BlockSpec((TILE, features), lambda i: (i, 0)),
        out_shape=jax.ShapeDtypeStruct((length, features), dtype),
        compiler_params=params(30),
        cost_estimate=COST,
        name="back",
    )(*[p.array for p in grads], *in_hbm([p.array for p in weights]), *add)


def norm_back(pairs, resid, gain, base, out_weights):
    n, m, (length, features) = len(pairs), len(out_weights), resid.shape
    grads, weights = zip(*pairs)
    tile = lambda x: Part(x).split(TILE)
    widths = [w.shape[0] for w in out_weights]
    return pl.pallas_call(
        functools.partial(back_kernel, n=n, m=m, norm=True, stacked=0),
        grid=(length // TILE,),
        in_specs=[g.split(TILE) for g in grads]
        + [w.spec() for w in weights]
        + [tile(resid), whole((1, features)), tile(base)]
        + [whole(w.shape) for w in out_weights],
        out_specs=[pl.BlockSpec((TILE, features), lambda i: (i, 0))] * 2
        + [whole((1, features))]
        + [pl.BlockSpec((TILE, w), lambda i: (i, 0)) for w in widths],
        out_shape=[
            jax.ShapeDtypeStruct((length, features), F32),
            jax.ShapeDtypeStruct((length, features), BF16),
            jax.ShapeDtypeStruct((1, features), F32),
        ]
        + [jax.ShapeDtypeStruct((length, w), BF16) for w in widths],
        compiler_params=params(34),
        cost_estimate=COST,
        name="norm_back",
    )(*[p.array for p in grads], *[p.array for p in weights], resid, gain.reshape(1, -1), base, *out_weights)


def weight_kernel(*refs, n, m):
    rows, grads, outs, turned = refs[:n], refs[n : n + m], refs[n + m : n + 2 * m], refs[-1]

    @pl.when(pl.program_id(0) == 0)
    def _():
        at = 0
        for ref in rows:
            for first in range(0, ref.shape[0], TILE):
                turned[:, at + first : at + first + TILE] = ref[first : first + TILE, :].astype(F32).T.astype(BF16)
            at += ref.shape[0]

    for grad, out in zip(grads, outs):
        out[...] = dot(turned[...], grad[...], 1, 0).astype(BF16)


def weight_grads(rows, grads, chunk):
    length, features = sum(x.shape[0] for x in rows), rows[0].shape[1]
    columns = grads[0].shape[1]
    return pl.pallas_call(
        functools.partial(weight_kernel, n=len(rows), m=len(grads)),
        grid=(columns // chunk,),
        in_specs=[whole(x.shape) for x in rows]
        + [pl.BlockSpec((length, chunk), lambda j: (0, j)) for _ in grads],
        out_specs=[pl.BlockSpec((features, chunk), lambda j: (0, j)) for _ in grads],
        out_shape=[jax.ShapeDtypeStruct((features, columns), BF16) for _ in grads],
        scratch_shapes=[pltpu.VMEM((features, length), BF16)],
        compiler_params=params(30),
        cost_estimate=COST,
        name="weight_grads",
    )(*rows, *grads)


def ffn_kernel(normed_ref, full_ref, gate_ref, up_ref, down_ref, hidden_ref, grads_ref, *, chunk, units):
    j = pl.program_id(0)
    gate = dot(normed_ref[...], gate_ref[...], 1, 0)
    up = dot(normed_ref[...], up_ref[...], 1, 0)
    hidden_grad = dot(full_ref[...], down_ref[...], 1, 1)
    act, slope = gelu_parts(gate)
    hidden_ref[...] = (act * up).astype(BF16)
    at = pl.multiple_of(j * chunk, chunk)
    grads_ref[:, pl.ds(at, chunk)] = (hidden_grad * up * slope).astype(BF16)
    grads_ref[:, pl.ds(pl.multiple_of(units + at, chunk), chunk)] = (hidden_grad * act).astype(BF16)


def feed_forward(normed, full, gate, up, down, chunk=256):
    (length, features), units = normed.shape, down.shape[0]

    def columns(part):
        if part.plane is None:
            first = part.at * part.columns // chunk
            return pl.BlockSpec((features, chunk), lambda j: (0, first + j))
        plane = part.plane
        return pl.BlockSpec((None, features, chunk), lambda j: (plane, 0, j))

    return pl.pallas_call(
        functools.partial(ffn_kernel, chunk=chunk, units=units),
        grid=(units // chunk,),
        in_specs=[
            whole(normed.shape),
            whole(full.shape),
            columns(gate),
            columns(up),
            pl.BlockSpec((chunk, features), lambda j: (j, 0)),
        ],
        out_specs=[pl.BlockSpec((length, chunk), lambda j: (0, j)), whole((length, 2 * units))],
        out_shape=[
            jax.ShapeDtypeStruct((length, units), BF16),
            jax.ShapeDtypeStruct((length, 2 * units), BF16),
        ],
        compiler_params=params(24),
        cost_estimate=COST,
        name="feed_forward",
    )(normed, full, *in_hbm([gate.array, up.array, down]))


def in_hbm(arrays):
    return [pltpu.with_memory_space_constraint(x, pltpu.HBM) for x in arrays]


def tie(x, *others):
    return lax.optimization_barrier((x, others))[0] if others else x


def arrange_kernel(scalars, mine_ref, theirs_ref, *out_refs, outputs):
    top = scalars[1]
    at = 0
    for out_ref, (width, planes) in zip(out_refs, outputs):
        for plane in range(max(planes, 1)):
            mine, theirs = (ref[0, :, at : at + width].astype(out_ref.dtype) for ref in (mine_ref, theirs_ref))
            at += width
            if planes:
                out_ref[plane, top, 0] = mine
                out_ref[plane, 1 - top, 0] = theirs
            else:
                out_ref[0, :, :width] = jnp.where(top == 0, mine, theirs)
                out_ref[0, :, width:] = jnp.where(top == 0, theirs, mine)


def arrange(mine, theirs, index, top, outputs, dtype):
    n, rows, columns = mine.shape
    scalars = jnp.stack([index, top]).astype(jnp.int32)
    specs, shapes = [], []
    for w, planes in outputs:
        if planes:
            specs.append(pl.BlockSpec((planes, 2, 1, rows, w), lambda i, sc: (0, 0, i, 0, 0)))
            shapes.append(jax.ShapeDtypeStruct((planes, 2, n, rows, w), dtype))
        else:
            specs.append(pl.BlockSpec((1, rows, 2 * w), lambda i, sc: (i, 0, 0)))
            shapes.append(jax.ShapeDtypeStruct((n, rows, 2 * w), dtype))
    outs = pl.pallas_call(
        functools.partial(arrange_kernel, outputs=outputs),
        grid_spec=pltpu.PrefetchScalarGridSpec(
            num_scalar_prefetch=1,
            grid=(n,),
            in_specs=[pl.BlockSpec((1, rows, columns), lambda i, sc: (i ^ sc[0], 0, 0))] * 2,
            out_specs=specs,
        ),
        out_shape=shapes,
        compiler_params=params(12),
        cost_estimate=COST,
        name="arrange",
    )(scalars, mine, theirs)
    return [
        x.reshape(x.shape[0], 2 * n * rows, w) if planes else x.reshape(n * rows, 2 * w)
        for x, (w, planes) in zip(outs, outputs)
    ]


class Links:
    def __init__(self, n_dp):
        self.n_dp = n_dp
        self.n_bits = n_dp.bit_length() - 1
        self.here = lax.axis_index("dp")

    def bit(self, k):
        return (self.here >> k) & 1

    def across_tp(self, x):
        return lax.ppermute(x, "tp", [(0, 1), (1, 0)])

    def across(self, x, mask):
        return lax.ppermute(x, "dp", [(i, i ^ mask) for i in range(self.n_dp)])


class Single:
    def __init__(self, move):
        self.move, self.started = move, False

    def send(self, x, *after):
        self.sent = tie(x, *after)
        self.got = [self.move(self.sent)]

    def take(self):
        return self.got[0]


class Fetch:
    def __init__(self, links, shards, bits, outputs):
        self.links, self.bits, self.outputs = links, list(bits), outputs
        self.n, self.index, self.got, self.held = 1 << len(bits), 0, None, None
        for place, k in enumerate(bits):
            self.index = self.index + (links.bit(k) << place)
        self.piece = jnp.concatenate([y for x in shards for y in self.pieces(x)], axis=2)

    def pieces(self, x):
        if isinstance(x, tuple):
            (x,) = x
            rows, columns, half = x.shape[0] * 2 // self.n, x.shape[1] // 2, self.n // 2
            at = (self.index % half * rows, self.index // half * columns)
            return [lax.dynamic_slice(x, at, (rows, columns))[None]]
        x = x.reshape(-1, self.n, x.shape[-2] // self.n, x.shape[-1])
        return list(lax.dynamic_slice_in_dim(x, self.index, 1, axis=1))

    def send(self, *after):
        if self.held is None:
            self.sent = tie(self.piece, *after)
            self.got = [self.links.across_tp(self.sent)]
        else:
            self.sent = tie(self.held, *after)
            self.got = [self.links.across(self.sent, 1 << self.bits[0])]

    def take(self):
        if self.held is None:
            self.held = self.got[0]
            return
        self.bits.pop(0)
        if self.bits:
            self.held = jnp.concatenate([self.held, self.got[0]], axis=0)
            if len(self.bits) == 1:
                self.last = self.bits[0]
        else:
            self.theirs = self.got[0]

    def ended(self):
        return not self.bits

    def finish(self):
        top, below = self.links.bit(self.last), self.index & (self.n // 2 - 1)
        whole_arrays = arrange(self.held, self.theirs, below, top, self.outputs, BF16)
        return [x[0] if x.ndim == 3 and x.shape[0] == 1 else x for x in whole_arrays]


TP = "tp"
HALO, PROJECT, MEMORY, GATE, DOWN, REST, CROSS, SELF = range(8)


class Reduction:
    def __init__(self, links, own, other, order, outputs):
        self.links, self.order, self.outputs = links, list(order), outputs
        self.back = [k for k in reversed(order) if k is not TP][:-1]
        self.n_blocks = links.n_dp
        view = lambda x: x.reshape(self.n_blocks, -1, x.shape[-1])
        self.own, self.other = [([view(x) for x in own], 0)], [([view(x) for x in other], 0)]
        self.at, self.size = 0, self.n_blocks
        self.index = 0
        self.result = self.theirs = None

    def piece(self, addends, at, size):
        total = 0.0
        for arrays, base in addends:
            parts = [lax.dynamic_slice_in_dim(x, at - base, size).astype(F32) for x in arrays]
            total = total + (jnp.concatenate(parts, axis=2) if len(parts) > 1 else parts[0])
        return total.astype(BF16)

    def send(self, *after):
        links = self.links
        if self.result is not None:
            bits = self.back[0] if self.back else (0,)
            masks = self.masks(bits)
            self.sent = tie(self.result, *after)
            self.got = [links.across(self.sent, mask) for mask in masks]
        elif self.order[0] is TP:
            self.sent = tie(self.piece(self.other, self.at, self.size), *after)
            self.got = [links.across_tp(self.sent)]
            self.other = None
        else:
            bits = self.order[0]
            masks = self.masks(bits)
            digit = 0
            for k in bits:
                digit = digit * 2 + links.bit(k)
            part = self.size // (len(masks) + 1)
            self.got, self.sent = [], []
            for i, mask in enumerate(masks):
                at = self.at + (digit ^ (i + 1)) * part
                sent = self.piece(self.own, at, part)
                if self.other is not None:
                    sent = jnp.concatenate([sent, self.piece(self.other, at, part)], axis=0)
                self.sent.append(tie(sent, *after))
                self.got.append(links.across(self.sent[-1], mask))
            self.at, self.size = self.at + digit * part, part
            if bits != (0,):
                self.index = self.index * (len(masks) + 1) + digit
        return self.got

    def masks(self, bits):
        out = []
        for i in range(1, 1 << len(bits)):
            out.append(sum(1 << k for place, k in enumerate(reversed(bits)) if (i >> place) & 1))
        return out

    def take(self):
        if self.result is not None:
            if self.back:
                self.back.pop(0)
                self.result = jnp.concatenate([self.result] + self.got, axis=0)
            else:
                self.theirs = self.got[0]
            return self.result
        self.order.pop(0)
        for got in self.got:
            self.own = self.own + [([got[: self.size]], self.at)]
            if self.other is not None:
                self.other = self.other + [([got[self.size :]], self.at)]
        if not self.order:
            self.result = self.piece(self.own, self.at, self.size)
        return self.got

    def ended(self):
        return self.theirs is not None

    def finish(self):
        return arrange(self.result, self.theirs, self.index, self.links.bit(0), self.outputs, F32)


class Agenda:
    def __init__(self, links):
        self.links, self.chains, self.now, self.strict = links, {}, (), True

    def at(self, x):
        return tie(x, *self.now)

    def after(self, *values):
        self.now = values

    def start(self, name, chain, *args):
        self.chains[name] = chain
        chain.send(*args, *self.now)
        self.now = (self.now, chain.sent)

    def go(self, name):
        chain = self.chains[name]
        if self.strict:
            chain.got = tie(chain.got, *self.now)
        came = chain.got
        chain.take()
        if chain.ended():
            self.now = (came,)
            return chain.finish()
        chain.send(came, *self.now)
        self.now = (came, chain.sent)

    def take(self, name):
        came = self.chains[name].take()
        if self.strict:
            came = tie(came, *self.now)
        self.now = (self.now, came)
        return came


def column_halves(x):
    half = x.shape[1] // 2
    return jnp.concatenate([x[:, :half], x[:, half:]], axis=0)


def beside(x):
    return jnp.concatenate(list(x), axis=1)


def shards(
    n_dp,
    decoder_rows,
    memory_rows,
    output_grad,
    token_segments,
    memory_segments,
    valid_mask,
    norm_gains,
    self_project,
    self_output,
    cross_query,
    cross_memory,
    cross_output,
    gate_up,
    down_weight,
):
    links = Links(n_dp)
    side = lax.axis_index("tp")
    decoder, memory, out_grad = decoder_rows[0], memory_rows[0], output_grad[0]
    valid = valid_mask[0]
    own_len, features = decoder.shape
    mem_len, columns = memory.shape[0], cross_query.shape[1]
    halo = token_segments.shape[1] // 4
    both = (0, 1)

    d, units = features, down_weight.shape[0]
    half_len = mem_len // 2
    agenda = Agenda(links)
    at, after, start, go, take = agenda.at, agenda.after, agenda.start, agenda.go, agenda.take
    v = types.SimpleNamespace()
    v.kv_own_of = [None, None]
    v.self_of = [None, None]
    v.cross_of = [None, None]
    v.query_grad_of = [None, None]
    v.kv_grad_of = [None, None]
    v.memory_dw_of = [None, None]
    v.proj_grad_of = [None, None]
    v.memory_came, v.memory_got = [], []
    bit0, bit1, rest = (0,), (1,), [(k,) for k in range(2, links.n_bits)]
    tp_first, tp_second, tp_third = (
        [bit0, TP, bit1] + rest,
        [bit0, bit1, TP] + rest,
        [bit0, bit1] + rest[:1] + [TP] + rest[1:],
    )
    resid0 = decoder.astype(F32)
    valid_rows = valid.astype(F32)[:, None]
    grad_m = out_grad.astype(F32) * valid_rows
    full_m = grad_m.astype(BF16)

    def sums(name, order, outputs, parts):
        after(parts)
        start(name, Reduction(links, *parts, order, outputs))

    def send_halo():
        start(HALO, Single(lambda x: lax.ppermute(x, "tp", [(0, 1)])), decoder[-halo:])

    def send_project():
        start(PROJECT, Fetch(links, [self_project], BITS, ((columns, 3),)))

    def send_memory(i):
        start(MEMORY, Single(links.across_tp), memory)

    def send_ffn():
        def mine(x):
            blocks = x.reshape(-1, links.n_dp, x.shape[-2] // links.n_dp, x.shape[-1])
            return jnp.concatenate(list(lax.dynamic_index_in_dim(blocks, links.here, 1, False)), axis=1)

        start(GATE, Single(links.across_tp), mine(gate_up))
        start(DOWN, Single(links.across_tp), mine(down_weight))

    def gather_ffn():
        gate_other = lax.all_gather(take(GATE), "dp", axis=0, tiled=True)
        v.gate_w = [Part(gate_up, plane=c) for c in both], [Part(gate_other, units, c) for c in both]
        v.down_w = (down_weight, lax.all_gather(take(DOWN), "dp", axis=0, tiled=True))

    def send_rest():
        start(
            REST,
            Fetch(
                links,
                [cross_memory, cross_query, (self_output,), (cross_output,)],
                BITS,
                ((columns, 2), (columns, 1), (columns, 0), (columns, 0)),
            ),
        )

    def plan():
        v.intervals = make_plans(side, token_segments, memory_segments, own_len, mem_len, halo)
        after(v.intervals)

    def norm_a():
        v.rows_a = jnp.concatenate([take(HALO), decoder], axis=0).astype(F32)
        v.normed_a = normalize(v.rows_a, norm_gains[0]).astype(BF16)

    def self_forward(h):
        if h:
            v.project = (self_project, out[PROJECT][0])
        weights = v.project[1] if h else self_project
        rows = at(v.normed_a)
        proj = [nn(rows, weights[c]).astype(BF16) for c in range(3)]
        att, totals = attend_forward(v.intervals, 0, columns, (proj[0], 0), ((proj[1], proj[2]),), halo)
        v.self_of[h] = proj, att, totals
        after(att)

    def keys_of(rows, h):
        return tuple(nn(rows, v.memory_w[h][c]).astype(BF16) for c in both)

    def keys_own(h):
        v.kv_own_of[h] = keys_of(at(memory), h)
        after(v.kv_own_of[h])

    def weights_rest():
        other_memory, other_query, other_out_a, other_out_c = out[REST]
        v.memory_w = (cross_memory, other_memory)
        v.out_a, v.out_c, v.query_w = (
            (self_output, other_out_a),
            (cross_output, other_out_c),
            (cross_query, other_query),
        )

    def queries():
        weights_rest()
        v.proj_a, v.att_a, v.totals_a = zip(*v.self_of)
        att = at(v.att_a)
        v.branch_a = nn(att[0], v.out_a[0]) + nn(att[1], v.out_a[1])
        v.resid1 = resid0 + v.branch_a
        v.normed_c = normalize(v.resid1, norm_gains[1]).astype(BF16)
        v.query_c = [nn(v.normed_c, v.query_w[h]).astype(BF16) for h in both]
        after(v.query_c)

    def take_memory():
        v.memory_came.append(take(MEMORY))

    def cross_forward(h):
        if not h:
            (v.memory_other,) = v.memory_came
        keys = (v.kv_own_of[h], keys_of(at(v.memory_other), h))
        att, totals = attend_forward(v.intervals, 1, columns, (v.query_c[h], 0), keys, 0)
        v.cross_of[h] = keys, att, totals
        after(att)

    def ffn():
        v.keys_c, v.att_c, v.totals_c = zip(*v.cross_of)
        att = at(v.att_c)
        v.branch_c = nn(att[0], v.out_c[0]) + nn(att[1], v.out_c[1])
        v.resid2 = v.resid1 + v.branch_c
        v.normed_m = normalize(v.resid2, norm_gains[2]).astype(BF16)
        v.hidden, v.gate_grads = zip(
            *[feed_forward(v.normed_m, full_m, *v.gate_w[h], v.down_w[h]) for h in both]
        )
        after(v.gate_grads)

    def gate_dw():
        agenda.strict = False
        parts = weight_grads([v.normed_m], at(list(v.gate_grads)), 512)
        sums(GATE, ORDERS[GATE], ((units, 2),), [[x] for x in parts])

    def down_dw():
        v.down_dw = weight_grads([at(full_m)], list(v.hidden), 512)
        after(v.down_dw)

    def norm_m_grad():
        v.gate_late = at(v.gate_grads)

    def norm_m_back():
        pairs = [(Part(v.gate_late[h], units, c), v.gate_w[h][c]) for h in both for c in both]
        v.grad_c, v.full_c, gain, *v.att_c_grad = norm_back(pairs, v.resid2, norm_gains[2], full_m, v.out_c)
        v.gain_m = gain[0]
        after(v.att_c_grad)

    def outs_dw():
        grad = at(v.full_c)
        out_dw = [weight_grads([v.att_c[h]], [grad], grad.shape[1])[0] for h in both]
        parts = [[v.down_dw[h], column_halves(out_dw[h])] for h in both]
        sums(DOWN, ORDERS[DOWN], ((units, 1), (columns, 0)), parts)

    def cross_backward(h):
        grad = at(v.att_c_grad[h])
        query = (v.query_c[h], 0)
        v.query_grad_of[h], v.kv_grad_of[h] = attend_backward(
            v.intervals, 1, columns, v.totals_c[h], query, v.att_c[h], grad, v.keys_c[h], 0, False
        )
        after(v.query_grad_of[h])

    def norm_c_back():
        grads = at(v.query_grad_of)
        pairs = [(Part(grads[h]), Part(v.query_w[h])) for h in both]
        v.grad_a, v.full_a, gain, *v.att_a_grad = norm_back(pairs, v.resid1, norm_gains[1], v.grad_c, v.out_a)
        v.gain_c = gain[0]
        after(v.att_a_grad)

    def memory_back(own):
        kv = at(v.kv_grad_of)
        row = 0 if own else mem_len
        pairs = [(Part(kv[h], columns, c, row=row), Part(v.memory_w[h], plane=c)) for h in both for c in both]
        if own:
            v.memory_grad = product_back(pairs, mem_len, F32, v.memory_got[0])
            after(v.memory_grad)
        else:
            v.memory_partial = product_back(pairs, mem_len, BF16)
            after(v.memory_partial)

    def send_partial(i):
        start(MEMORY, Single(links.across_tp), v.memory_partial)

    def take_partial():
        v.memory_got.append(take(MEMORY))

    def memory_dw(h):
        if h:
            v.memory_dw_of = weight_grads([memory, v.memory_other], at(v.kv_grad_of), 384)
            after(v.memory_dw_of)

    def cross_dw():
        query_dw = weight_grads([at(v.normed_c)], v.query_grad_of, columns)
        out_dw = [weight_grads([v.att_a[h]], [at(v.full_a)], v.full_a.shape[1])[0] for h in both]
        parts = [[v.memory_dw_of[h], query_dw[h], column_halves(out_dw[h])] for h in both]
        sums(CROSS, ORDERS[CROSS], ((columns, 2), (columns, 1), (columns, 0)), parts)

    def self_backward(h):
        grad = at(v.att_a_grad[h])
        proj, *keys = v.proj_a[h]
        v.proj_grad_of[h] = attend_backward(
            v.intervals, 0, columns, v.totals_a[h], (proj, 0), v.att_a[h], grad, (keys,), halo, True
        )[0]
        after(v.proj_grad_of[h])

    def norm_a_grad():
        grads = at(v.proj_grad_of)
        pairs = [(Part(grads[h], columns, c), Part(v.project[h], plane=c)) for h in both for c in range(3)]
        v.normed_a_grad = total = product_back(pairs, own_len + halo, F32)
        after(total)
        start(HALO, Single(lambda x: lax.ppermute(x, "tp", [(1, 0)])), total[:halo].astype(BF16))
        v.branch_m = nn(v.hidden[0], v.down_w[0]) + nn(v.hidden[1], v.down_w[1])
        v.result = v.resid2 + v.branch_m
        gain_a = jnp.sum(total * v.rows_a * inverse_rms(v.rows_a), axis=0)
        rows = [jnp.sum(x * x * valid_rows, axis=0) for x in (v.result, v.branch_a, v.branch_c, v.branch_m)]
        rows += [jnp.sum(jnp.broadcast_to(valid_rows, resid0.shape), axis=0), v.gain_m, v.gain_c, gain_a]
        v.stats = jnp.pad(jnp.stack(rows), ((0, 2 * HD - len(rows)), (0, 0))).T.astype(BF16)

    def self_dw():
        parts = [[x, v.stats] for x in weight_grads([v.normed_a], at(v.proj_grad_of), 384)]
        sums(SELF, ORDERS[SELF], ((columns, 3), (2 * HD, 1)), parts)

    def norm_a_back():
        came = take(HALO).astype(F32)
        own = at(v.normed_a_grad[halo:])
        own = jnp.concatenate([own[:-halo], own[-halo:] + came], axis=0)
        resid0_grad, _ = normalize_back(resid0, norm_gains[0], own)
        v.decoder_grad = v.grad_a + resid0_grad
        after(v.decoder_grad)

    BITS = (1, 0)
    ORDERS = {GATE: tp_first, DOWN: tp_second, CROSS: tp_second, SELF: tp_first}
    v.memory_w = (None, None)
    out = {}

    def keys_first():
        v.memory_w = (cross_memory, None)
        keys_own(0)

    def advance(name):
        came = go(name)
        if came is not None:
            if name == DOWN:
                came[0] = came[0][0].T
            out[name] = came
            after(came)

    def for_each(block):
        return [functools.partial(block, h) for h in both]

    mem0, mem1 = for_each(send_memory)
    self0, self1 = for_each(self_forward)
    keys0, keys1 = keys_first, functools.partial(keys_own, 1)
    cross0, cross1 = for_each(cross_forward)
    cross_b0, cross_b1 = for_each(cross_backward)
    part0, part1 = for_each(send_partial)
    mem_dw0, mem_dw1 = for_each(memory_dw)
    self_b0, self_b1 = for_each(self_backward)
    mem_b0, mem_b1 = for_each(memory_back)
    P_, R, A, B, E, D = [functools.partial(advance, name) for name in (PROJECT, REST, GATE, DOWN, CROSS, SELF)]
    agenda_steps = (
        send_halo, send_project, send_ffn, plan, norm_a, P_, gather_ffn, send_rest, self0, P_, mem0, R, keys0, P_,
        self1, R, R, take_memory, queries, keys1, cross0, cross1, ffn, gate_dw, down_dw, norm_m_grad, A, norm_m_back,
        outs_dw, cross_b0, B, cross_b1, A, norm_c_back, B, mem_b0, part0, mem_dw0, mem_dw1, cross_dw, A, B, self_b1,
        E, A, B, self_b0, A, B, norm_a_grad, self_dw, E, A, B, take_partial, D, mem_b1, A, B, norm_a_back, E, D, A, B,
        E, D, A, E, D, B, E, D, E, D, E, D, E, D, D,
    )
    for step in agenda_steps:
        step()
    for name in (GATE, DOWN, CROSS, SELF):
        while name not in out:
            advance(name)

    stats = out[SELF][1][0, :, :8].T
    gains_grad = jnp.stack([stats[7], stats[6], stats[5]])
    root_squares = jnp.sqrt(jnp.sum(stats[:4], axis=1) / jnp.sum(stats[4]))
    return (
        v.result.astype(BF16)[None],
        v.decoder_grad[None],
        v.memory_grad[None],
        root_squares,
        gains_grad,
        out[SELF][0],
        out[CROSS][2],
        out[CROSS][1][0],
        out[CROSS][0],
        out[DOWN][1],
        out[GATE][0],
        out[DOWN][0],
    )


def solution(mesh):
    assert mesh.shape["tp"] == 2
    return jax.shard_map(
        functools.partial(shards, mesh.shape["dp"]),
        mesh=mesh,
        in_specs=(
            P("dp", "tp", None),
            P("dp", "tp", None),
            P("dp", "tp", None),
            P("dp", None),
            P("dp", None),
            P("dp", "tp"),
            P(),
            P(None, None, "tp"),
            P("tp", None),
            P(None, "tp"),
            P(None, None, "tp"),
            P("tp", None),
            P(None, None, "tp"),
            P("tp", None),
        ),
        out_specs=(
            P("dp", "tp", None),
            P("dp", "tp", None),
            P("dp", "tp", None),
            P(),
            P(),
            P(None, None, "tp"),
            P("tp", None),
            P(None, "tp"),
            P(None, None, "tp"),
            P("tp", None),
            P(None, None, "tp"),
            P("tp", None),
        ),
        check_vma=False,
    )
```
